256 devices in a mesh: slab: 8 (over z_lo, x), grp: 32 (over y, z_hi, core).
Axes of the slice: x: 4, y: 4, z: 8 (z_hi: 4, z_lo: 2; z = z_hi * 2 + z_lo), core: 2. Of those that a mesh axis runs over, the one named last changes fastest.
Arguments:
- blocks: bfloat16 [1024, 9, 256, 256], P(('slab', 'grp')), may hold values from -0.75 to 0.75
- diag_shift: float32 [262144], P(('slab', 'grp')), may hold values from 1 to 16
- offsets: int32 [1024, 2], P(('slab', 'grp')), may hold values from 0 to 4
Outputs:
- factors: bfloat16 [1024, 9, 256, 256], P(('slab', 'grp'))
The draws below stay inside these ranges and needn't reach their ends.
Inputs may be any that keep to these rules, and one draw needn't show every extreme that they name: offsets[i, 0] bounds from above the pattern's blocks left of the diagonal block of block row i and offsets[i, 1] those right of it; blocks that would lie outside the matrix are not in the pattern.
All inputs are finite; a program needn't handle non-finite values.
Results may differ from the reference program's by a relative error of at most 0.001.
Values may be sent and summed in bfloat16 or wider, within the bound.
A program may use at most 256 MiB of HBM per device.

```python
import math
import jax
import jax.numpy as jnp
from jax import lax

B = 256
BW = 4
RB = 4
ITERS = 2
NBR = 1024
N_SLAB = 8
N_GRP = 32


def touch_ends(drawn, rng, least, high):
    place = [jax.random.randint(jax.random.fold_in(rng, axis), (), 0, length) for axis, length in enumerate(drawn.shape)]
    main_axis = drawn.shape.index(max(drawn.shape))
    next_to = place[:main_axis] + [(place[main_axis] + 1) % drawn.shape[main_axis]] + place[main_axis + 1:]
    return drawn.at[tuple(place)].set(least).at[tuple(next_to)].set(high)


def steps_of(stream_key, dims, split, low, largest):
    level, own = 1.0, jax.random.fold_in(stream_key, 6)
    for dim, blocks in split:
        steps = jnp.exp(jax.random.uniform(jax.random.fold_in(own, dim), (blocks,), jnp.float32, low / len(split), largest / len(split)))
        level = level * jnp.repeat(steps, dims[dim] // blocks).reshape([-1 if axis == dim else 1 for axis in range(len(dims))])
    return level


def bell_draw(rng, dims, width, reach, split=(), held_as=jnp.bfloat16):
    gain = steps_of(rng, dims, split, -0.22, 0.18) if split else 1.0
    drawn = jax.random.normal(rng, dims, jnp.float32) * width * gain
    return jnp.minimum(jnp.maximum(drawn, -reach), reach).astype(held_as)


def setup_inputs(seed: int = 0) -> dict:
    key_of = jax.random.split(jax.random.key(seed), 4)
    return {
        "blocks": bell_draw(key_of[0], (NBR, 2 * BW + 1, B, B), 0.05, 0.75, ((0, 256),)),
        "diag_shift": jnp.clip(jnp.exp(math.log(16.0) - 2.7725887 * jax.random.uniform(key_of[1], (NBR * B,), jnp.float32) ** steps_of(key_of[1], (NBR * B,), ((0, 256),), -0.2, 0.2)), 1.0, 16.0),
        "offsets": touch_ends(jax.random.randint(key_of[2], (NBR, 2), 0, BW + 1), jax.random.fold_in(key_of[2], 1), 0, BW).astype(jnp.int32),
    }


def band_pattern(global_rows, offsets, band_count, all_rows):
    band_reach = (band_count - 1) // 2
    relative = jnp.arange(band_count, dtype=jnp.int32) - band_reach
    lower_count = offsets[:, 0:1]
    upper_count = offsets[:, 1:2]
    target = global_rows[:, None] + relative[None, :]
    left_side = (relative < 0) & (-relative <= lower_count) & (target >= 0)
    right_side = (relative > 0) & (relative <= upper_count) & (target < all_rows)
    return (relative == 0) | left_side | right_side

def new_rows(factors_now, above_rows, scaled, present):
    band_count = factors_now.shape[1]
    band_reach = (band_count - 1) // 2
    row_count = factors_now.shape[0]
    block_size = factors_now.shape[2]
    partial_value = scaled.astype(jnp.float32)
    for offset_back in range(1, band_reach + 1):
        left_block = factors_now[:, band_reach - offset_back].astype(jnp.float32)
        upper_rows = above_rows[band_reach - offset_back:band_reach - offset_back + row_count, 1:].astype(jnp.float32)
        product = jnp.einsum('rab,rsbc->rsac', left_block, upper_rows)
        partial_value = partial_value.at[:, band_reach - offset_back + 1:2 * band_reach - offset_back + 1].add(-product)
    pieces = []
    for offset_back in range(band_reach, 0, -1):
        pivot_block = above_rows[band_reach - offset_back:band_reach - offset_back + row_count, 0].astype(jnp.float32)
        strict = jnp.triu(pivot_block, 1)
        inner_term = jnp.einsum('rab,rbc->rac', factors_now[:, band_reach - offset_back].astype(jnp.float32), strict)
        diag_values = jnp.diagonal(pivot_block, axis1=1, axis2=2)
        divisor = jnp.where(present[:, band_reach - offset_back][:, None], diag_values, 1.0)
        pieces.append((partial_value[:, band_reach - offset_back] - inner_term) / divisor[:, None, :])
    own_block = factors_now[:, band_reach].astype(jnp.float32)
    strict_lower = jnp.tril(own_block, -1)
    diag_rest = partial_value[:, band_reach] - jnp.einsum('rab,rbc->rac', strict_lower, jnp.triu(own_block, 1))
    own_diag = jnp.diagonal(own_block, axis1=1, axis2=2)
    below_mask = jnp.tril(jnp.ones((block_size, block_size), jnp.int32), -1) > 0
    pieces.append(jnp.where(below_mask[None], diag_rest / own_diag[:, None, :], diag_rest))
    upper_terms = partial_value[:, band_reach + 1:] - jnp.einsum('rab,rsbc->rsac', strict_lower, factors_now[:, band_reach + 1:].astype(jnp.float32))
    stacked = jnp.concatenate([jnp.stack(pieces, 1), upper_terms], 1)
    return jnp.where(present[:, :, None, None], stacked, 0.0).astype(jnp.bfloat16)

def reference(blocks, diag_shift, offsets):
    row_total, band_count, block_size, _ = blocks.shape
    band_reach = (band_count - 1) // 2
    shift_rows = diag_shift.reshape(row_total, block_size)
    diag_values = shift_rows + jnp.diagonal(blocks[:, band_reach].astype(jnp.float32), axis1=1, axis2=2)
    padded = jnp.pad(diag_values, ((band_reach, band_reach), (0, 0)))
    positive = padded > 0
    scales = jnp.where(positive, 1.0 / jnp.sqrt(jnp.where(positive, padded, 1.0)), 0.0)
    row_scale = scales[band_reach:band_reach + row_total]
    col_scale = jnp.stack([scales[column:column + row_total] for column in range(band_count)], 1)
    present = band_pattern(jnp.arange(row_total, dtype=jnp.int32), offsets, band_count, row_total)
    group_count = row_total // RB
    identity = jnp.eye(block_size, dtype=jnp.float32)

    def scale_group(index):
        start = (index * RB).astype(jnp.int32)
        piece = lax.dynamic_slice_in_dim(blocks, start, RB, 0).astype(jnp.float32)
        added = lax.dynamic_slice_in_dim(shift_rows, start, RB, 0)
        piece = piece.at[:, band_reach].add(identity[None] * added[:, None, :])
        rscale = lax.dynamic_slice_in_dim(row_scale, start, RB, 0)
        cscale = lax.dynamic_slice_in_dim(col_scale, start, RB, 0)
        marks = lax.dynamic_slice_in_dim(present, start, RB, 0)
        value = piece * rscale[:, None, :, None] * cscale[:, :, None, :]
        return jnp.where(marks[:, :, None, None], value, 0.0).astype(jnp.bfloat16)
    scaled = lax.map(scale_group, jnp.arange(group_count, dtype=jnp.int32)).reshape(blocks.shape)
    padded_state = jnp.concatenate([jnp.zeros((band_reach,) + blocks.shape[1:], jnp.bfloat16), scaled], 0)
    slab_rows = N_GRP * RB

    def slab_update(slab_index, padded_state):
        slab_start = (slab_index * slab_rows).astype(jnp.int32)

        def group_update(group_index):
            start = (slab_start + group_index * RB).astype(jnp.int32)
            current = lax.dynamic_slice_in_dim(padded_state, start + band_reach, RB, 0)
            above_rows = lax.dynamic_slice_in_dim(padded_state, start, RB + band_reach, 0)[:, band_reach:]
            return new_rows(current, above_rows, lax.dynamic_slice_in_dim(scaled, start, RB, 0), lax.dynamic_slice_in_dim(present, start, RB, 0))
        fresh = lax.map(group_update, jnp.arange(N_GRP, dtype=jnp.int32)).reshape((slab_rows,) + blocks.shape[1:])
        return lax.dynamic_update_slice_in_dim(padded_state, fresh, (slab_start + band_reach).astype(jnp.int32), 0)
    for sweep_index in range(ITERS):
        padded_state = lax.fori_loop(0, N_SLAB, slab_update, padded_state)
    return padded_state[band_reach:]
```

```python
import functools

import jax
import jax.numpy as jnp
from jax import lax
from jax.experimental import pallas as pl
from jax.experimental.pallas import tpu as pltpu
from jax.sharding import PartitionSpec as P

MESH = pl.DeviceIdType.MESH
F32 = jnp.float32
BF16 = jnp.bfloat16
BW = 4
LANES = 128


def mm(lhs, rhs):
    lhs = lhs[0] if len(lhs) == 1 else jnp.concatenate(lhs, axis=1)
    rhs = rhs[0] if len(rhs) == 1 else jnp.concatenate(rhs, axis=0)
    return jnp.dot(lhs, rhs, preferred_element_type=F32)


def kernel(
    n_slab, n_grp,
    blocks, shift, offs, out,
    w0, l0, w1, l1, wo, lo,
    base, msg, above, below, reach, sc, rs, rd,
    in_sem, out_sem, m_send, m_recv, x_send, x_recv, y_send, y_recv, q_send, q_recv,
):
    rows, _, size, _ = blocks.shape
    half = size // 2
    slab, grp = lax.axis_index("slab"), lax.axis_index("grp")
    flat = slab * n_grp + grp
    total = n_slab * n_grp
    has_prev, has_next = flat > 0, flat < total - 1
    after, before = jnp.minimum(flat + 1, total - 1), jnp.maximum(flat - 1, 0)
    nxt = (after // n_grp, after % n_grp)
    prv = (before // n_grp, before % n_grp)
    inside = grp < n_grp - 1
    edge_out = jnp.logical_and(has_next, grp == n_grp - 1)
    edge_in = jnp.logical_and(has_prev, grp == 0)

    def remote(src, dst, send, recv, where_to):
        return pltpu.make_async_remote_copy(
            src_ref=src, dst_ref=dst, send_sem=send, recv_sem=recv, device_id=where_to, device_id_type=MESH
        )

    loads = [
        pltpu.make_async_copy(blocks.at[:, BW], w0.at[pl.ds(BW, rows), 0], in_sem.at[0]),
        pltpu.make_async_copy(blocks.at[:, pl.ds(BW + 1, BW)], w0.at[pl.ds(BW, rows), pl.ds(1, BW)], in_sem.at[1]),
        pltpu.make_async_copy(blocks.at[:, pl.ds(0, BW)], l0, in_sem.at[2]),
    ]
    for load in loads:
        load.start()

    barrier = pltpu.get_barrier_semaphore()

    @pl.when(has_next)
    def _():
        pl.semaphore_signal(barrier, inc=1, device_id=nxt, device_id_type=MESH)

    @pl.when(has_prev)
    def _():
        pl.semaphore_signal(barrier, inc=1, device_id=prv, device_id_type=MESH)

    pl.semaphore_wait(barrier, has_next.astype(jnp.int32) + has_prev.astype(jnp.int32))

    def x_parts(source):
        parts = []
        for r in range(rows - 1, -1, -1):
            first, count = BW - r, r + 1
            parts.append(remote(source(r, first, count), w0.at[r, pl.ds(first, count)], x_send.at[r], x_recv.at[r], nxt))
        for r in range(rows - 1, -1, -1):
            count = BW - r
            at = rows + r
            parts.append(remote(source(r, 0, count), w0.at[r, pl.ds(0, count)], x_send.at[at], x_recv.at[at], nxt))
        return parts

    def y_part(row_ref, r, kind):
        at = r * 4 + kind
        dst = w1.at[r]
        if kind == 0:
            cut = (pl.ds(BW - r, r),)
        elif kind == 1:
            cut = (pl.ds(1, BW - 1 - r),)
        elif kind == 2:
            cut = (0, pl.ds(0, half))
        else:
            cut = (0, pl.ds(half, half), pl.ds(half, half))
        return remote(row_ref.at[cut], dst.at[cut], y_send.at[at], y_recv.at[at], nxt)

    def y_parts(source):
        order = [(r, 0) for r in range(rows - 1, 0, -1)]
        for r in range(rows - 1, -1, -1):
            order += [(r, 1)] * (r < rows - 1) + [(r, 2), (r, 3)]
        return [y_part(source(r), r, kind) for r, kind in order]

    from_input = x_parts(lambda r, first, count: blocks.at[r, pl.ds(BW + first, count)])
    from_first = x_parts(lambda r, first, count: w1.at[BW + r, pl.ds(first, count)])
    q_copy = remote(blocks.at[:, 2 * BW], base, q_send, q_recv, nxt)

    @pl.when(inside)
    def _():
        for part in from_input:
            part.start()

    @pl.when(edge_out)
    def _():
        q_copy.start()

    @pl.when(jnp.logical_not(has_prev))
    def _():
        above[...] = jnp.zeros_like(above)

        def clear(i, c):
            a, t = i // (BW + 1), i % (BW + 1)
            w0[a, t] = jnp.zeros((size, size), BF16)
            w1[a, t] = jnp.zeros((size, size), BF16)
            return c

        lax.fori_loop(0, BW * (BW + 1), clear, 0)

    @pl.when(jnp.logical_not(has_next))
    def _():
        below[...] = jnp.zeros_like(below)

    row_id = lax.broadcasted_iota(jnp.int32, (size, size), 0)
    col_id = lax.broadcasted_iota(jnp.int32, (size, size), 1)
    eye = row_id == col_id

    def diagonal(block):
        return jnp.sum(jnp.where(eye, block.astype(F32), 0.0), axis=0, keepdims=True)

    loads[0].wait()
    for r in range(rows):
        msg[pl.ds(r, 1), :] = shift[pl.ds(r, 1), :] + diagonal(w0[BW + r, 0])
        at = flat * rows + r
        up = jnp.minimum(offs[r, 1], total * rows - 1 - at)
        down = jnp.minimum(offs[r, 0], at)
        msg[pl.ds(rows + r, 1), :] = jnp.broadcast_to(up.astype(F32), (1, size))
        reach[pl.ds(r, 1), :] = jnp.broadcast_to(down.astype(F32), (1, size))
    to_next = remote(msg, above, m_send.at[0], m_recv.at[0], nxt)
    to_prev = remote(msg, below, m_send.at[1], m_recv.at[1], prv)

    @pl.when(has_next)
    def _():
        to_next.start()

    @pl.when(has_prev)
    def _():
        to_prev.start()

    loads[1].wait()
    loads[2].wait()

    @pl.when(has_prev)
    def _():
        to_next.wait_recv()

    @pl.when(has_next)
    def _():
        to_prev.wait_recv()

    def scale_of(values):
        positive = values > 0
        return jnp.where(positive, 1.0 / jnp.sqrt(jnp.where(positive, values, 1.0)), 0.0)

    sc[pl.ds(0, rows), :] = scale_of(above[pl.ds(0, rows), :])
    sc[pl.ds(rows, rows), :] = scale_of(msg[pl.ds(0, rows), :])
    sc[pl.ds(2 * rows, rows), :] = scale_of(below[pl.ds(0, rows), :])

    def spread(j, c):
        column = jnp.sum(jnp.where(eye, jnp.broadcast_to(sc[pl.ds(j, 1), :], (size, size)), 0.0), axis=1, keepdims=True)
        rs[j] = jnp.broadcast_to(column, (size, LANES))
        return c

    lax.fori_loop(0, 2 * rows, spread, 0)

    def scaled(block, j, column, keep):
        row_scale = jnp.concatenate([rs[j]] * (size // LANES), axis=1)
        value = block.astype(F32) * row_scale * sc[pl.ds(column, 1), :]
        return jnp.where(jnp.broadcast_to(keep, (size, size)), value, 0.0).astype(BF16)

    def scaled_diag(block, j, values):
        row_scale = jnp.concatenate([rs[j]] * (size // LANES), axis=1)
        full = jnp.where(eye, jnp.broadcast_to(values, (size, size)), block.astype(F32))
        return (full * row_scale * sc[pl.ds(j, 1), :]).astype(BF16)

    def own_upper(i, c):
        r, t = i // BW, 1 + i % BW
        keep = msg[pl.ds(rows + r, 1), :] >= t.astype(F32)
        w0[BW + r, t] = scaled(w0[BW + r, t], BW + r, BW + r + t, keep)
        return c

    def own_lower(i, c):
        r, k = i // BW, i % BW
        keep = reach[pl.ds(r, 1), :] >= (BW - k).astype(F32)
        l0[r, k] = scaled(l0[r, k], BW + r, r + k, keep)
        return c

    def own_diag(r, c):
        w0[BW + r, 0] = scaled_diag(w0[BW + r, 0], BW + r, msg[pl.ds(r, 1), :])
        return c

    lax.fori_loop(0, rows, own_diag, 0)
    lax.fori_loop(0, rows * BW, own_upper, 0)
    lax.fori_loop(0, rows * BW, own_lower, 0)

    def above_upper(a):
        def step(t, c):
            keep = above[pl.ds(rows + a, 1), :] >= t.astype(F32)
            w0[a, t] = scaled(w0[a, t], a, a + t, keep)
            return c

        return step

    strict_up, strict_low = col_id > row_id, row_id > col_id

    def keep_if(mask, block):
        return jnp.where(mask, block.astype(F32), 0.0).astype(BF16)

    def upper_row(r, w, l, w_new, new_row):
        own = w[BW + r, 0]
        low = keep_if(strict_low, own)
        pivot = 1.0 / diagonal(own)
        rd[pl.ds(BW + r, 1), :] = pivot
        for t in range(BW + 1):
            lhs, rhs = [low], [keep_if(strict_up, own) if t == 0 else w[BW + r, t]]
            for m in range(1, BW + 1 - t):
                lhs.append(l[r, BW - m])
                rhs.append(w[BW + r - m, t + m])
            value = w0[BW + r, t].astype(F32) - mm(lhs, rhs)
            if t == 0:
                value = jnp.where(strict_low, value * pivot, value)
            else:
                keep = msg[pl.ds(rows + r, 1), :] >= float(t)
                value = jnp.where(jnp.broadcast_to(keep, (size, size)), value, 0.0)
            w_new[new_row, t] = value.astype(BF16)

    def lower_row(r, w, l, l_new):
        for k in range(BW):
            m = BW - k
            lhs, rhs = [l[r, k]], [keep_if(strict_up, w[BW + r - m, 0])]
            for back in range(m + 1, BW + 1):
                lhs.append(l[r, BW - back])
                rhs.append(w[BW + r - back, back - m])
            value = (l0[r, k].astype(F32) - mm(lhs, rhs)) * rd[pl.ds(BW + r - m, 1), :]
            keep = reach[pl.ds(r, 1), :] >= float(m)
            l_new[r, k] = jnp.where(jnp.broadcast_to(keep, (size, size)), value, 0.0).astype(BF16)

    def arrive(r, pieces):
        for c in range(rows):

            @pl.when(jnp.logical_and(has_prev, r == c))
            def _():
                for piece in pieces[c]:
                    piece.wait_recv()

    x_first = [[p] for p in reversed(from_input[:rows])]
    x_rest = [[p] for p in reversed(from_input[rows:])]
    y_first = [[y_part(w1.at[BW + r], r, 0)] if r else [] for r in range(rows)]
    y_rest = [
        [y_part(w1.at[BW + r], r, kind) for kind in ((1, 2, 3) if r < rows - 1 else (2, 3))] for r in range(rows)
    ]

    @pl.when(edge_in)
    def _():
        q_copy.wait_recv()

    def upper_1(i, c):
        r = rows - 1 - i
        arrive(r, x_first)

        @pl.when(grp > 0)
        def _():
            lax.fori_loop(BW - r, BW + 1, above_upper(r), 0)
            base[r] = w0[r, BW]

        @pl.when(grp == 0)
        def _():
            keep = above[pl.ds(rows + r, 1), :] >= float(BW)
            base[r] = scaled(base[r], r, r + BW, keep)

        upper_row(r, w0, l0, w1, BW + r)
        return c

    @pl.when(jnp.logical_not(has_prev))
    def _():
        def clear(a, c):
            base[a] = jnp.zeros((size, size), BF16)
            return c

        lax.fori_loop(0, rows, clear, 0)

    lax.fori_loop(0, rows, upper_1, 0)

    @pl.when(inside)
    def _():
        for part in y_parts(lambda r: w1.at[BW + r]):
            part.start()

    @pl.when(edge_out)
    def _():
        for part in from_first:
            part.start()

    def lower_1(i, c):
        r = rows - 1 - i
        arrive(r, x_rest)

        @pl.when(grp > 0)
        def _():
            w0[r, 0] = scaled_diag(w0[r, 0], r, above[pl.ds(r, 1), :])
            lax.fori_loop(1, BW - r, above_upper(r), 0)

        rd[pl.ds(r, 1), :] = 1.0 / diagonal(w0[r, 0])
        lower_row(r, w0, l0, l1)
        return c

    lax.fori_loop(0, rows, lower_1, 0)

    outs_up = [pltpu.make_async_copy(wo.at[r], out.at[r, pl.ds(BW, BW + 1)], out_sem.at[r]) for r in range(rows)]
    outs_low = [pltpu.make_async_copy(lo.at[r], out.at[r, pl.ds(0, BW)], out_sem.at[rows + r]) for r in range(rows)]

    def leave(r, copies):
        for c in range(rows):

            @pl.when(r == c)
            def _():
                copies[c].start()

    def upper_2(i, c):
        r = rows - 1 - i
        arrive(r, y_first)
        keep = above[pl.ds(rows + r, 1), :] >= float(BW)
        value = base[r].astype(F32) - mm([keep_if(strict_low, w0[r, 0])], [w0[r, BW]])
        w1[r, BW] = jnp.where(jnp.broadcast_to(keep, (size, size)), value, 0.0).astype(BF16)
        upper_row(r, w1, l1, wo, r)
        return c

    lax.fori_loop(0, rows, upper_2, 0)

    @pl.when(edge_out)
    def _():
        for part in y_parts(lambda r: wo.at[r]):
            part.start()

    for copy in outs_up:
        copy.start()

    def lower_2(i, c):
        r = rows - 1 - i
        arrive(r, y_rest)
        rd[pl.ds(r, 1), :] = 1.0 / diagonal(w1[r, 0])
        lower_row(r, w1, l1, lo)
        leave(r, outs_low)
        return c

    lax.fori_loop(0, rows, lower_2, 0)

    @pl.when(has_next)
    def _():
        for part in from_input + y_parts(lambda r: w1.at[BW + r]) + [to_next]:
            part.wait_send()

    @pl.when(edge_out)
    def _():
        q_copy.wait_send()

    @pl.when(has_prev)
    def _():
        to_prev.wait_send()

    for copy in outs_up + outs_low:
        copy.wait()


def per_device(n_slab, n_grp, blocks, diag_shift, offsets):
    rows, band, size, _ = blocks.shape
    block = (size, size)
    call = pl.pallas_call(
        functools.partial(kernel, n_slab, n_grp),
        out_shape=jax.ShapeDtypeStruct(blocks.shape, BF16),
        in_specs=[
            pl.BlockSpec(memory_space=pl.ANY),
            pl.BlockSpec(memory_space=pltpu.VMEM),
            pl.BlockSpec(memory_space=pltpu.SMEM),
        ],
        out_specs=pl.BlockSpec(memory_space=pl.ANY),
        scratch_shapes=[
            pltpu.VMEM((2 * rows, BW + 1) + block, BF16),
            pltpu.VMEM((rows, BW) + block, BF16),
            pltpu.VMEM((2 * rows, BW + 1) + block, BF16),
            pltpu.VMEM((rows, BW) + block, BF16),
            pltpu.VMEM((rows, BW + 1) + block, BF16),
            pltpu.VMEM((rows, BW) + block, BF16),
            pltpu.VMEM((rows,) + block, BF16),
            pltpu.VMEM((2 * rows, size), F32),
            pltpu.VMEM((2 * rows, size), F32),
            pltpu.VMEM((2 * rows, size), F32),
            pltpu.VMEM((2 * rows, size), F32),
            pltpu.VMEM((4 * rows, size), F32),
            pltpu.VMEM((2 * rows, size, LANES), F32),
            pltpu.VMEM((2 * rows, size), F32),
            pltpu.SemaphoreType.DMA((3,)),
            pltpu.SemaphoreType.DMA((2 * rows,)),
            pltpu.SemaphoreType.DMA((2,)),
            pltpu.SemaphoreType.DMA((2,)),
            pltpu.SemaphoreType.DMA((2 * rows,)),
            pltpu.SemaphoreType.DMA((2 * rows,)),
            pltpu.SemaphoreType.DMA((4 * rows,)),
            pltpu.SemaphoreType.DMA((4 * rows,)),
            pltpu.SemaphoreType.DMA,
            pltpu.SemaphoreType.DMA,
        ],
        compiler_params=pltpu.CompilerParams(
            collective_id=0, has_side_effects=True, vmem_limit_bytes=60 * 1024 * 1024
        ),
        name="sweeps",
    )
    return call(blocks, diag_shift.reshape(rows, size), offsets)


def solution(mesh):
    return jax.shard_map(
        functools.partial(per_device, mesh.shape["slab"], mesh.shape["grp"]),
        mesh=mesh,
        in_specs=(
            P(("slab", "grp"), None, None, None),
            P(("slab", "grp")),
            P(("slab", "grp"), None),
        ),
        out_specs=P(("slab", "grp"), None, None, None),
        check_vma=False,
    )
```

```python
import functools

import jax
import jax.numpy as jnp
from jax import lax
from jax.experimental import pallas as pl
from jax.experimental.pallas import tpu as pltpu
from jax.sharding import PartitionSpec as P

MESH = pl.DeviceIdType.MESH
F32 = jnp.float32
BF16 = jnp.bfloat16
BW = 4
LANES = 128
DIRECT = 2


def mm(lhs, rhs):
    lhs = lhs[0] if len(lhs) == 1 else jnp.concatenate(lhs, axis=1)
    rhs = rhs[0] if len(rhs) == 1 else jnp.concatenate(rhs, axis=0)
    return jnp.dot(lhs, rhs, preferred_element_type=F32)


def kernel(
    n_slab, n_grp,
    blocks, shift, offs, out,
    w0, l0, w1, l1, wo, lo,
    base, diag0, relay, msg, above, below, reach, sc, rs, rd,
    in_sem, out_sem, m_send, m_recv, x_send, x_recv, y_send, y_recv, q_send, q_recv,
    o_send, o_recv, r_send, r_recv,
):
    rows, _, size, _ = blocks.shape
    half = size // 2
    slab, grp = lax.axis_index("slab"), lax.axis_index("grp")
    flat = slab * n_grp + grp
    total = n_slab * n_grp
    has_prev, has_next = flat > 0, flat < total - 1
    after, before = jnp.minimum(flat + 1, total - 1), jnp.maximum(flat - 1, 0)
    nxt = (after // n_grp, after % n_grp)
    prv = (before // n_grp, before % n_grp)

    n_x, n_zh = n_slab // 2, min(4, n_grp // 2)
    odd = grp % 2 == 1

    def along_z(place, step):
        slab_at, grp_at = place
        z = (grp_at // 2 % n_zh * 2 + slab_at // n_x + step + 4 * n_zh) % (2 * n_zh)
        return (z % 2 * n_x + slab_at % n_x, grp_at // (2 * n_zh) * (2 * n_zh) + z // 2 * 2 + grp_at % 2)

    my_relay = along_z((slab, grp), -3)
    origin = along_z((slab, grp), 3)
    prv_relay = along_z(prv, -3)
    origin_flat = origin[0] * n_grp + origin[1]
    target_flat = jnp.minimum(origin_flat + 1, total - 1)
    target = (target_flat // n_grp, target_flat % n_grp)
    relaying = jnp.logical_and(odd, origin_flat < total - 1)
    origin_edge = jnp.logical_and(relaying, origin[1] == n_grp - 1)
    inside = grp < n_grp - 1
    edge_out = jnp.logical_and(has_next, grp == n_grp - 1)
    edge_in = jnp.logical_and(has_prev, grp == 0)

    def remote(src, dst, send, recv, where_to):
        return pltpu.make_async_remote_copy(
            src_ref=src, dst_ref=dst, send_sem=send, recv_sem=recv, device_id=where_to, device_id_type=MESH
        )

    loads = [
        pltpu.make_async_copy(blocks.at[:, BW], w0.at[pl.ds(BW, rows), 0], in_sem.at[0]),
        pltpu.make_async_copy(blocks.at[:, pl.ds(BW + 1, BW)], w0.at[pl.ds(BW, rows), pl.ds(1, BW)], in_sem.at[1]),
        pltpu.make_async_copy(blocks.at[:, pl.ds(0, BW)], l0, in_sem.at[2]),
    ]
    for load in loads:
        load.start()

    barrier = pltpu.get_barrier_semaphore()

    @pl.when(has_next)
    def _():
        pl.semaphore_signal(barrier, inc=1, device_id=nxt, device_id_type=MESH)

    @pl.when(has_prev)
    def _():
        pl.semaphore_signal(barrier, inc=1, device_id=prv, device_id_type=MESH)

    @pl.when(odd)
    def _():
        pl.semaphore_signal(barrier, inc=1, device_id=origin, device_id_type=MESH)

    from_relay = jnp.logical_and(has_prev, jnp.logical_not(odd))

    @pl.when(from_relay)
    def _():
        pl.semaphore_signal(barrier, inc=1, device_id=prv_relay, device_id_type=MESH)

    one = jnp.int32(1)
    peers = sum(jnp.where(c, one, 0) for c in (has_next, has_prev, odd, relaying))
    pl.semaphore_wait(barrier, peers)

    def x_crit(source, r, last):
        first = BW - r
        cut = pl.ds(first, last - first)
        return remote(source(r, first, last - first), w0.at[r, cut], x_send.at[r], x_recv.at[r], nxt)

    def x_rest(source, r, first, last):
        cut = pl.ds(first, last - first)
        at = rows + r
        return remote(source(r, first, last - first), w0.at[r, cut], x_send.at[at], x_recv.at[at], nxt)

    downward = list(range(rows - 1, -1, -1))
    rest = [(r, t) for r in downward for t in range(BW - r)]
    n_out = len(rest) - DIRECT

    def out_copy(j, source):
        r, t = rest[j]
        return remote(source(r, t, 1), relay.at[pl.ds(j, 1)], o_send.at[j], o_recv.at[j], my_relay)

    def on_copy(j):
        r, t = rest[j]
        return remote(relay.at[pl.ds(j, 1)], w0.at[r, pl.ds(t, 1)], r_send.at[j], r_recv.at[j], target)

    def forward(js):
        for j in js:

            @pl.when(relaying if j < n_out else origin_edge)
            def _():
                out_copy(j, from_first).wait_recv()
                on_copy(j).start()

    def y_part(row_ref, r, kind):
        at = r * 4 + kind
        dst = w1.at[r]
        if kind == 0:
            cut = (pl.ds(BW - r, r),)
        elif kind == 1:
            cut = (pl.ds(1, BW - 1 - r),)
        elif kind == 2:
            cut = (0, pl.ds(0, half))
        else:
            cut = (0, pl.ds(half, half), pl.ds(half, half))
        return remote(row_ref.at[cut], dst.at[cut], y_send.at[at], y_recv.at[at], nxt)

    def y_parts(source):
        order = [(r, 0) for r in range(rows - 1, 0, -1)]
        for r in range(rows - 1, -1, -1):
            order += [(r, 1)] * (r < rows - 1) + [(r, 2), (r, 3)]
        return [y_part(source(r), r, kind) for r, kind in order]

    def from_input(r, first, count):
        return blocks.at[r, pl.ds(BW + first, count)]

    def from_first(r, first, count):
        return w1.at[BW + r, pl.ds(first, count)]

    inside_odd = jnp.logical_and(inside, odd)
    q_copy = remote(blocks.at[:, 2 * BW], base, q_send.at[0], q_recv.at[0], nxt)
    g_copy = remote(blocks.at[:, BW], diag0, q_send.at[1], q_recv.at[1], nxt)

    @pl.when(inside)
    def _():
        for r in downward:
            x_crit(from_input, r, BW + 1).start()

    @pl.when(inside_odd)
    def _():
        for j in range(n_out):
            out_copy(j, from_input).start()
        if DIRECT:
            x_rest(from_input, 0, BW - DIRECT, BW).start()

    @pl.when(jnp.logical_not(odd))
    def _():
        for r in downward:
            x_rest(from_input, r, 0, BW - r).start()

    @pl.when(edge_out)
    def _():
        q_copy.start()
        g_copy.start()

    @pl.when(jnp.logical_not(has_prev))
    def _():
        above[...] = jnp.zeros_like(above)

        def clear(i, c):
            a, t = i // (BW + 1), i % (BW + 1)
            w0[a, t] = jnp.zeros((size, size), BF16)
            w1[a, t] = jnp.zeros((size, size), BF16)
            return c

        lax.fori_loop(0, BW * (BW + 1), clear, 0)

    @pl.when(jnp.logical_not(has_next))
    def _():
        below[...] = jnp.zeros_like(below)

    row_id = lax.broadcasted_iota(jnp.int32, (size, size), 0)
    col_id = lax.broadcasted_iota(jnp.int32, (size, size), 1)
    eye = row_id == col_id

    def diagonal(block):
        return jnp.sum(jnp.where(eye, block.astype(F32), 0.0), axis=0, keepdims=True)

    loads[0].wait()
    for r in range(rows):
        msg[pl.ds(r, 1), :] = shift[pl.ds(r, 1), :] + diagonal(w0[BW + r, 0])
        at = flat * rows + r
        up = jnp.minimum(offs[r, 1], total * rows - 1 - at)
        down = jnp.minimum(offs[r, 0], at)
        msg[pl.ds(rows + r, 1), :] = jnp.broadcast_to(up.astype(F32), (1, size))
        reach[pl.ds(r, 1), :] = jnp.broadcast_to(down.astype(F32), (1, size))
    to_next = remote(msg, above, m_send.at[0], m_recv.at[0], nxt)
    to_prev = remote(msg, below, m_send.at[1], m_recv.at[1], prv)

    @pl.when(has_next)
    def _():
        to_next.start()

    @pl.when(has_prev)
    def _():
        to_prev.start()

    loads[1].wait()
    loads[2].wait()

    @pl.when(has_prev)
    def _():
        to_next.wait_recv()

    @pl.when(has_next)
    def _():
        to_prev.wait_recv()

    def scale_of(values):
        positive = values > 0
        return jnp.where(positive, 1.0 / jnp.sqrt(jnp.where(positive, values, 1.0)), 0.0)

    sc[pl.ds(0, rows), :] = scale_of(above[pl.ds(0, rows), :])
    sc[pl.ds(rows, rows), :] = scale_of(msg[pl.ds(0, rows), :])
    sc[pl.ds(2 * rows, rows), :] = scale_of(below[pl.ds(0, rows), :])

    def spread(j, c):
        column = jnp.sum(jnp.where(eye, jnp.broadcast_to(sc[pl.ds(j, 1), :], (size, size)), 0.0), axis=1, keepdims=True)
        rs[j] = jnp.broadcast_to(column, (size, LANES))
        return c

    lax.fori_loop(0, 2 * rows, spread, 0)

    def scaled(block, j, column, keep):
        row_scale = jnp.concatenate([rs[j]] * (size // LANES), axis=1)
        value = block.astype(F32) * row_scale * sc[pl.ds(column, 1), :]
        return jnp.where(jnp.broadcast_to(keep, (size, size)), value, 0.0).astype(BF16)

    def scaled_diag(block, j, values):
        row_scale = jnp.concatenate([rs[j]] * (size // LANES), axis=1)
        full = jnp.where(eye, jnp.broadcast_to(values, (size, size)), block.astype(F32))
        return (full * row_scale * sc[pl.ds(j, 1), :]).astype(BF16)

    def own_upper(i, c):
        r, t = i // BW, 1 + i % BW
        keep = msg[pl.ds(rows + r, 1), :] >= t.astype(F32)
        w0[BW + r, t] = scaled(w0[BW + r, t], BW + r, BW + r + t, keep)
        return c

    def own_lower(i, c):
        r, k = i // BW, i % BW
        keep = reach[pl.ds(r, 1), :] >= (BW - k).astype(F32)
        l0[r, k] = scaled(l0[r, k], BW + r, r + k, keep)
        return c

    def own_diag(r, c):
        w0[BW + r, 0] = scaled_diag(w0[BW + r, 0], BW + r, msg[pl.ds(r, 1), :])
        return c

    lax.fori_loop(0, rows, own_diag, 0)
    lax.fori_loop(0, rows * BW, own_upper, 0)
    lax.fori_loop(0, rows * BW, own_lower, 0)

    def above_upper(a):
        def step(t, c):
            keep = above[pl.ds(rows + a, 1), :] >= t.astype(F32)
            w0[a, t] = scaled(w0[a, t], a, a + t, keep)
            return c

        return step

    strict_up, strict_low = col_id > row_id, row_id > col_id

    def keep_if(mask, block):
        return jnp.where(mask, block.astype(F32), 0.0).astype(BF16)

    def upper_row(r, w, l, w_new, new_row):
        own = w[BW + r, 0]
        low = keep_if(strict_low, own)
        pivot = 1.0 / diagonal(own)
        rd[pl.ds(BW + r, 1), :] = pivot
        for t in range(BW + 1):
            lhs, rhs = [low], [keep_if(strict_up, own) if t == 0 else w[BW + r, t]]
            for m in range(1, BW + 1 - t):
                lhs.append(l[r, BW - m])
                rhs.append(w[BW + r - m, t + m])
            value = w0[BW + r, t].astype(F32) - mm(lhs, rhs)
            if t == 0:
                value = jnp.where(strict_low, value * pivot, value)
            else:
                keep = msg[pl.ds(rows + r, 1), :] >= float(t)
                value = jnp.where(jnp.broadcast_to(keep, (size, size)), value, 0.0)
            w_new[new_row, t] = value.astype(BF16)

    def lower_row(r, w, l, l_new):
        for k in range(BW):
            m = BW - k
            lhs, rhs = [l[r, k]], [keep_if(strict_up, w[BW + r - m, 0])]
            for back in range(m + 1, BW + 1):
                lhs.append(l[r, BW - back])
                rhs.append(w[BW + r - back, back - m])
            value = (l0[r, k].astype(F32) - mm(lhs, rhs)) * rd[pl.ds(BW + r - m, 1), :]
            keep = reach[pl.ds(r, 1), :] >= float(m)
            l_new[r, k] = jnp.where(jnp.broadcast_to(keep, (size, size)), value, 0.0).astype(BF16)

    def arrive(r, pieces, when):
        for c in range(rows):
            if pieces[c]:

                @pl.when(jnp.logical_and(when, r == c))
                def _():
                    for piece in pieces[c]:
                        piece.wait_recv()

    relayed = [[on_copy(j) for j in range(n_out) if rest[j][0] == r] for r in range(rows)]
    relayed_edge = [[on_copy(j) for j in range(n_out, len(rest)) if rest[j][0] == r] for r in range(rows)]
    direct_rest = [[x_rest(from_first, 0, BW - DIRECT, BW)] if DIRECT and r == 0 else [] for r in range(rows)]
    beside_rest = [[x_rest(from_first, r, 0, BW - r)] for r in range(rows)]
    x_first = [[x_crit(from_first, r, BW + 1)] for r in range(rows)]
    x_first_edge = [[x_crit(from_first, r, BW)] if r else [] for r in range(rows)]
    y_first = [[y_part(w1.at[BW + r], r, 0)] if r else [] for r in range(rows)]
    y_rest = [
        [y_part(w1.at[BW + r], r, kind) for kind in ((1, 2, 3) if r < rows - 1 else (2, 3))] for r in range(rows)
    ]

    @pl.when(edge_in)
    def _():
        q_copy.wait_recv()
        g_copy.wait_recv()

    def last_column(r, diag_block, old):
        keep = above[pl.ds(rows + r, 1), :] >= float(BW)
        value = base[r].astype(F32) - mm([keep_if(strict_low, diag_block)], [old])
        return jnp.where(jnp.broadcast_to(keep, (size, size)), value, 0.0).astype(BF16)

    def upper_1(i, c):
        r = rows - 1 - i
        arrive(r, x_first, grp > 0)
        arrive(r, x_first_edge, edge_in)

        @pl.when(grp > 0)
        def _():
            lax.fori_loop(BW - r, BW + 1, above_upper(r), 0)
            base[r] = w0[r, BW]

        @pl.when(grp == 0)
        def _():
            keep = above[pl.ds(rows + r, 1), :] >= float(BW)
            base[r] = scaled(base[r], r, r + BW, keep)
            first_diag = scaled_diag(diag0[r], r, above[pl.ds(r, 1), :])
            w0[r, BW] = last_column(r, first_diag, base[r])

        upper_row(r, w0, l0, w1, BW + r)
        return c

    @pl.when(jnp.logical_not(has_prev))
    def _():
        def clear(a, c):
            base[a] = jnp.zeros((size, size), BF16)
            diag0[a] = jnp.zeros((size, size), BF16)
            return c

        lax.fori_loop(0, rows, clear, 0)

    lax.fori_loop(0, rows, upper_1, 0)

    @pl.when(inside)
    def _():
        for part in y_parts(lambda r: w1.at[BW + r]):
            part.start()

    @pl.when(edge_out)
    def _():
        for r in range(rows - 1, 0, -1):
            x_crit(from_first, r, BW).start()
        for j in range(len(rest)):
            out_copy(j, from_first).start()

    def lower_1(i, c):
        r = rows - 1 - i
        arrive(r, beside_rest, odd)
        arrive(r, relayed, from_relay)
        arrive(r, relayed_edge, edge_in)
        arrive(r, direct_rest, jnp.logical_and(from_relay, grp > 0))

        @pl.when(grp > 0)
        def _():
            w0[r, 0] = scaled_diag(w0[r, 0], r, above[pl.ds(r, 1), :])
            lax.fori_loop(1, BW - r, above_upper(r), 0)

        rd[pl.ds(r, 1), :] = 1.0 / diagonal(w0[r, 0])
        lower_row(r, w0, l0, l1)
        return c

    lax.fori_loop(0, rows, lower_1, 0)

    half_way = len(rest) // 2
    forward(range(half_way))

    @pl.when(grp < n_grp - 1)
    def _():
        forward(range(half_way, len(rest)))

    outs_up = [pltpu.make_async_copy(wo.at[r], out.at[r, pl.ds(BW, BW + 1)], out_sem.at[r]) for r in range(rows)]
    outs_low = [pltpu.make_async_copy(lo.at[r], out.at[r, pl.ds(0, BW)], out_sem.at[rows + r]) for r in range(rows)]

    def leave(r, copies):
        for c in range(rows):

            @pl.when(r == c)
            def _():
                copies[c].start()

    def upper_2(i, c):
        r = rows - 1 - i
        arrive(r, y_first, has_prev)
        w1[r, BW] = last_column(r, w0[r, 0], w0[r, BW])
        upper_row(r, w1, l1, wo, r)
        return c

    lax.fori_loop(0, rows, upper_2, 0)

    @pl.when(edge_out)
    def _():
        for part in y_parts(lambda r: wo.at[r]):
            part.start()

    @pl.when(grp == n_grp - 1)
    def _():
        forward(range(half_way, len(rest)))

    for copy in outs_up:
        copy.start()

    def lower_2(i, c):
        r = rows - 1 - i
        arrive(r, y_rest, has_prev)
        rd[pl.ds(r, 1), :] = 1.0 / diagonal(w1[r, 0])
        lower_row(r, w1, l1, lo)
        leave(r, outs_low)
        return c

    lax.fori_loop(0, rows, lower_2, 0)

    @pl.when(has_next)
    def _():
        for part in y_parts(lambda r: w1.at[BW + r]) + [to_next]:
            part.wait_send()

    @pl.when(inside)
    def _():
        for r in downward:
            x_crit(from_first, r, BW + 1).wait_send()

    @pl.when(jnp.logical_not(odd))
    def _():
        for r in downward:
            x_rest(from_first, r, 0, BW - r).wait_send()

    @pl.when(inside_odd)
    def _():
        for j in range(n_out):
            out_copy(j, from_first).wait_send()
        if DIRECT:
            x_rest(from_first, 0, BW - DIRECT, BW).wait_send()

    @pl.when(edge_out)
    def _():
        q_copy.wait_send()
        g_copy.wait_send()
        for r in range(rows - 1, 0, -1):
            x_crit(from_first, r, BW).wait_send()
        for j in range(len(rest)):
            out_copy(j, from_first).wait_send()

    for j in range(len(rest)):

        @pl.when(relaying if j < n_out else origin_edge)
        def _():
            on_copy(j).wait_send()

    @pl.when(has_prev)
    def _():
        to_prev.wait_send()

    for copy in outs_up + outs_low:
        copy.wait()


def per_device(n_slab, n_grp, blocks, diag_shift, offsets):
    rows, band, size, _ = blocks.shape
    block = (size, size)
    n_rest = BW * (BW + 1) // 2
    call = pl.pallas_call(
        functools.partial(kernel, n_slab, n_grp),
        out_shape=jax.ShapeDtypeStruct(blocks.shape, BF16),
        in_specs=[
            pl.BlockSpec(memory_space=pl.ANY),
            pl.BlockSpec(memory_space=pltpu.VMEM),
            pl.BlockSpec(memory_space=pltpu.SMEM),
        ],
        out_specs=pl.BlockSpec(memory_space=pl.ANY),
        scratch_shapes=[
            pltpu.VMEM((2 * rows, BW + 1) + block, BF16),
            pltpu.VMEM((rows, BW) + block, BF16),
            pltpu.VMEM((2 * rows, BW + 1) + block, BF16),
            pltpu.VMEM((rows, BW) + block, BF16),
            pltpu.VMEM((rows, BW + 1) + block, BF16),
            pltpu.VMEM((rows, BW) + block, BF16),
            pltpu.VMEM((rows,) + block, BF16),
            pltpu.VMEM((rows,) + block, BF16),
            pltpu.VMEM((n_rest,) + block, BF16),
            pltpu.VMEM((2 * rows, size), F32),
            pltpu.VMEM((2 * rows, size), F32),
            pltpu.VMEM((2 * rows, size), F32),
            pltpu.VMEM((2 * rows, size), F32),
            pltpu.VMEM((4 * rows, size), F32),
            pltpu.VMEM((2 * rows, size, LANES), F32),
            pltpu.VMEM((2 * rows, size), F32),
            pltpu.SemaphoreType.DMA((3,)),
            pltpu.SemaphoreType.DMA((2 * rows,)),
            pltpu.SemaphoreType.DMA((2,)),
            pltpu.SemaphoreType.DMA((2,)),
            pltpu.SemaphoreType.DMA((2 * rows,)),
            pltpu.SemaphoreType.DMA((2 * rows,)),
            pltpu.SemaphoreType.DMA((4 * rows,)),
            pltpu.SemaphoreType.DMA((4 * rows,)),
            pltpu.SemaphoreType.DMA((2,)),
            pltpu.SemaphoreType.DMA((2,)),
        ] + [pltpu.SemaphoreType.DMA((n_rest,))] * 4,
        compiler_params=pltpu.CompilerParams(
            collective_id=0, has_side_effects=True, vmem_limit_bytes=60 * 1024 * 1024
        ),
        name="sweeps",
    )
    return call(blocks, diag_shift.reshape(rows, size), offsets)


def solution(mesh):
    return jax.shard_map(
        functools.partial(per_device, mesh.shape["slab"], mesh.shape["grp"]),
        mesh=mesh,
        in_specs=(
            P(("slab", "grp"), None, None, None),
            P(("slab", "grp")),
            P(("slab", "grp"), None),
        ),
        out_specs=P(("slab", "grp"), None, None, None),
        check_vma=False,
    )
```

```python
import functools

import jax
import jax.numpy as jnp
from jax import lax
from jax.experimental import pallas as pl
from jax.experimental.pallas import tpu as pltpu
from jax.sharding import PartitionSpec as P

MESH = pl.DeviceIdType.MESH
F32 = jnp.float32
BF16 = jnp.bfloat16
BW = 4
LANES = 128
DIRECT = 2


def mm(lhs, rhs):
    lhs = lhs[0] if len(lhs) == 1 else jnp.concatenate(lhs, axis=1)
    rhs = rhs[0] if len(rhs) == 1 else jnp.concatenate(rhs, axis=0)
    return jnp.dot(lhs, rhs, preferred_element_type=F32)


def kernel(
    n_slab, n_grp,
    blocks, shift_in, offs_in, out,
    w0, l0, w1, l1,
    base, diag0, relay, shift, offs, msg, above, below, reach, sc, rs, rd,
    in_sem, m_send, m_recv, x_send, x_recv, y_send, y_recv, g_send, g_recv,
    o_send, o_recv, r_send, r_recv,
):
    rows, _, size, _ = blocks.shape
    wo, lo = out.at[:, pl.ds(BW, BW + 1)], out.at[:, pl.ds(0, BW)]
    half = size // 2
    slab, grp = lax.axis_index("slab"), lax.axis_index("grp")
    flat = slab * n_grp + grp
    total = n_slab * n_grp
    has_prev, has_next = flat > 0, flat < total - 1
    after, before = jnp.minimum(flat + 1, total - 1), jnp.maximum(flat - 1, 0)
    nxt = (after // n_grp, after % n_grp)
    prv = (before // n_grp, before % n_grp)

    n_x, n_zh = n_slab // 2, min(4, n_grp // 2)
    odd = grp % 2 == 1

    def along_z(place, step):
        slab_at, grp_at = place
        z = (grp_at // 2 % n_zh * 2 + slab_at // n_x + step + 4 * n_zh) % (2 * n_zh)
        return (z % 2 * n_x + slab_at % n_x, grp_at // (2 * n_zh) * (2 * n_zh) + z // 2 * 2 + grp_at % 2)

    my_relay = along_z((slab, grp), -3)
    origin = along_z((slab, grp), 3)
    prv_relay = along_z(prv, -3)
    origin_flat = origin[0] * n_grp + origin[1]
    target_flat = jnp.minimum(origin_flat + 1, total - 1)
    target = (target_flat // n_grp, target_flat % n_grp)
    relaying = jnp.logical_and(odd, origin_flat < total - 1)
    origin_edge = jnp.logical_and(relaying, origin[1] == n_grp - 1)
    inside = grp < n_grp - 1
    edge_out = jnp.logical_and(has_next, grp == n_grp - 1)
    edge_in = jnp.logical_and(has_prev, grp == 0)

    def remote(src, dst, send, recv, where_to):
        return pltpu.make_async_remote_copy(
            src_ref=src, dst_ref=dst, send_sem=send, recv_sem=recv, device_id=where_to, device_id_type=MESH
        )

    loads = [
        pltpu.make_async_copy(blocks.at[:, BW], w0.at[pl.ds(BW, rows), 0], in_sem.at[0]),
        pltpu.make_async_copy(blocks.at[:, pl.ds(BW + 1, BW)], w0.at[pl.ds(BW, rows), pl.ds(1, BW)], in_sem.at[1]),
        pltpu.make_async_copy(blocks.at[:, pl.ds(0, BW)], l0, in_sem.at[2]),
        pltpu.make_async_copy(shift_in, shift, in_sem.at[3]),
        pltpu.make_async_copy(offs_in, offs, in_sem.at[4]),
    ]
    for load in loads:
        load.start()

    barrier = pltpu.get_barrier_semaphore()

    @pl.when(has_next)
    def _():
        pl.semaphore_signal(barrier, inc=1, device_id=nxt, device_id_type=MESH)

    @pl.when(has_prev)
    def _():
        pl.semaphore_signal(barrier, inc=1, device_id=prv, device_id_type=MESH)

    @pl.when(odd)
    def _():
        pl.semaphore_signal(barrier, inc=1, device_id=origin, device_id_type=MESH)

    from_relay = jnp.logical_and(has_prev, jnp.logical_not(odd))

    @pl.when(from_relay)
    def _():
        pl.semaphore_signal(barrier, inc=1, device_id=prv_relay, device_id_type=MESH)

    one = jnp.int32(1)
    peers = sum(jnp.where(c, one, 0) for c in (has_next, has_prev, odd, relaying))
    pl.semaphore_wait(barrier, peers)

    def x_crit(source, r, last):
        first = BW - r
        cut = pl.ds(first, last - first)
        return remote(source(r, first, last - first), w0.at[r, cut], x_send.at[r], x_recv.at[r], nxt)

    def x_rest(source, r, first, last):
        cut = pl.ds(first, last - first)
        at = rows + r
        return remote(source(r, first, last - first), w0.at[r, cut], x_send.at[at], x_recv.at[at], nxt)

    def from_input(r, first, count):
        return blocks.at[r, pl.ds(BW + first, count)]

    def from_first(r, first, count):
        return w1.at[BW + r, pl.ds(first, count)]

    downward = list(range(rows - 1, -1, -1))
    rest = [(r, t) for r in downward for t in range(BW - r)]
    by_relay = rest[: len(rest) - DIRECT]
    by_relay_edge = [(r, -1) for r in downward] + [(r, t) for r, t in rest if r > 0]
    n_plain, n_edge = len(by_relay), len(by_relay_edge)

    def out_copy(j, edge, source=from_first):
        r, t = by_relay_edge[j] if edge else by_relay[j]
        src = blocks.at[r, pl.ds(2 * BW, 1)] if t < 0 else source(r, t, 1)
        return remote(src, relay.at[pl.ds(j, 1)], o_send.at[j], o_recv.at[j], my_relay)

    def on_copy(j, edge):
        r, t = by_relay_edge[j] if edge else by_relay[j]
        dst = base.at[pl.ds(r, 1)] if t < 0 else w0.at[r, pl.ds(t, 1)]
        return remote(relay.at[pl.ds(j, 1)], dst, r_send.at[j], r_recv.at[j], target)

    relaying_plain = jnp.logical_and(relaying, jnp.logical_not(origin_edge))

    def forward(js):
        for j in js:
            if j < n_plain:

                @pl.when(relaying_plain)
                def _():
                    out_copy(j, False).wait_recv()
                    on_copy(j, False).start()

            @pl.when(origin_edge)
            def _():
                out_copy(j, True).wait_recv()
                on_copy(j, True).start()

    def y_part(row_ref, r, kind):
        at = r * 4 + kind
        dst = w1.at[r]
        if kind == 0:
            cut = (pl.ds(BW - r, r),)
        elif kind == 1:
            cut = (pl.ds(1, BW - 1 - r),)
        elif kind == 2:
            cut = (0, pl.ds(0, half))
        else:
            cut = (0, pl.ds(half, half), pl.ds(half, half))
        return remote(row_ref.at[cut], dst.at[cut], y_send.at[at], y_recv.at[at], nxt)

    def y_parts(source):
        order = [(r, 0) for r in range(rows - 1, 0, -1)]
        for r in range(rows - 1, -1, -1):
            order += [(r, 1)] * (r < rows - 1) + [(r, 2), (r, 3)]
        return [y_part(source(r), r, kind) for r, kind in order]

    inside_odd = jnp.logical_and(inside, odd)
    half_rows = pl.ds(half, half)
    g_copies = [
        remote(blocks.at[:, BW, half_rows], diag0.at[:, half_rows], g_send.at[0], g_recv.at[0], nxt),
        remote(
            blocks.at[:, BW, pl.ds(0, half), pl.ds(0, half)],
            diag0.at[:, pl.ds(0, half), pl.ds(0, half)],
            g_send.at[1], g_recv.at[1], nxt,
        ),
    ]

    @pl.when(inside_odd)
    def _():
        for j in range(n_plain):
            out_copy(j, False, from_input).start()

    @pl.when(edge_out)
    def _():
        for j in range(rows):
            out_copy(j, True).start()

    @pl.when(jnp.logical_not(has_prev))
    def _():
        above[...] = jnp.zeros_like(above)

        def clear(i, c):
            a, t = i // (BW + 1), i % (BW + 1)
            w0[a, t] = jnp.zeros((size, size), BF16)
            w1[a, t] = jnp.zeros((size, size), BF16)
            return c

        lax.fori_loop(0, BW * (BW + 1), clear, 0)

    @pl.when(jnp.logical_not(has_next))
    def _():
        below[...] = jnp.zeros_like(below)

    row_id = lax.broadcasted_iota(jnp.int32, (size, size), 0)
    col_id = lax.broadcasted_iota(jnp.int32, (size, size), 1)
    eye = row_id == col_id

    def diagonal(block):
        return jnp.sum(jnp.where(eye, block.astype(F32), 0.0), axis=0, keepdims=True)

    loads[0].wait()
    loads[3].wait()
    loads[4].wait()
    reaches = offs[...]
    for r in range(rows):
        msg[pl.ds(r, 1), :] = shift[pl.ds(r * size, size)].reshape(1, size) + diagonal(w0[BW + r, 0])
        at = flat * rows + r
        up = jnp.minimum(reaches[1:2, r : r + 1], total * rows - 1 - at)
        down = jnp.minimum(reaches[0:1, r : r + 1], at)
        msg[pl.ds(rows + r, 1), :] = jnp.broadcast_to(up.astype(F32), (1, size))
        reach[pl.ds(r, 1), :] = jnp.broadcast_to(down.astype(F32), (1, size))
    to_next = remote(msg, above, m_send.at[0], m_recv.at[0], nxt)
    to_prev = remote(msg, below, m_send.at[1], m_recv.at[1], prv)

    @pl.when(has_next)
    def _():
        to_next.start()

    @pl.when(has_prev)
    def _():
        to_prev.start()

    @pl.when(inside)
    def _():
        for r in downward:
            x_crit(from_input, r, BW + 1).start()

    @pl.when(inside_odd)
    def _():
        x_rest(from_input, 0, BW - DIRECT, BW).start()

    @pl.when(jnp.logical_not(odd))
    def _():
        for r in downward:
            x_rest(from_input, r, 0, BW - r).start()

    @pl.when(edge_out)
    def _():
        for copy in g_copies:
            copy.start()

    loads[1].wait()
    loads[2].wait()

    @pl.when(has_prev)
    def _():
        to_next.wait_recv()

    @pl.when(has_next)
    def _():
        to_prev.wait_recv()

    def scale_of(values):
        positive = values > 0
        return jnp.where(positive, 1.0 / jnp.sqrt(jnp.where(positive, values, 1.0)), 0.0)

    sc[pl.ds(0, rows), :] = scale_of(above[pl.ds(0, rows), :])
    sc[pl.ds(rows, rows), :] = scale_of(msg[pl.ds(0, rows), :])
    sc[pl.ds(2 * rows, rows), :] = scale_of(below[pl.ds(0, rows), :])

    def spread(j, c):
        column = jnp.sum(jnp.where(eye, jnp.broadcast_to(sc[pl.ds(j, 1), :], (size, size)), 0.0), axis=1, keepdims=True)
        rs[j] = jnp.broadcast_to(column, (size, LANES))
        return c

    lax.fori_loop(0, 2 * rows, spread, 0)

    def scaled(block, j, column, keep):
        row_scale = jnp.concatenate([rs[j]] * (size // LANES), axis=1)
        value = block.astype(F32) * row_scale * sc[pl.ds(column, 1), :]
        return jnp.where(jnp.broadcast_to(keep, (size, size)), value, 0.0).astype(BF16)

    def scaled_diag(block, j, values):
        row_scale = jnp.concatenate([rs[j]] * (size // LANES), axis=1)
        full = jnp.where(eye, jnp.broadcast_to(values, (size, size)), block.astype(F32))
        return (full * row_scale * sc[pl.ds(j, 1), :]).astype(BF16)

    def own_upper(i, c):
        r, t = i // BW, 1 + i % BW
        keep = msg[pl.ds(rows + r, 1), :] >= t.astype(F32)
        w0[BW + r, t] = scaled(w0[BW + r, t], BW + r, BW + r + t, keep)
        return c

    def own_lower(i, c):
        r, k = i // BW, i % BW
        keep = reach[pl.ds(r, 1), :] >= (BW - k).astype(F32)
        l0[r, k] = scaled(l0[r, k], BW + r, r + k, keep)
        return c

    def own_diag(r, c):
        w0[BW + r, 0] = scaled_diag(w0[BW + r, 0], BW + r, msg[pl.ds(r, 1), :])
        return c

    lax.fori_loop(0, rows, own_diag, 0)
    lax.fori_loop(0, rows * BW, own_upper, 0)
    lax.fori_loop(0, rows * BW, own_lower, 0)

    def above_upper(a):
        def step(t, c):
            keep = above[pl.ds(rows + a, 1), :] >= t.astype(F32)
            w0[a, t] = scaled(w0[a, t], a, a + t, keep)
            return c

        return step

    strict_up, strict_low = col_id > row_id, row_id > col_id

    def keep_if(mask, block):
        return jnp.where(mask, block.astype(F32), 0.0).astype(BF16)

    def upper_row(r, w, l, w_new, new_row):
        own = w[BW + r, 0]
        low = keep_if(strict_low, own)
        pivot = 1.0 / diagonal(own)
        rd[pl.ds(BW + r, 1), :] = pivot
        for t in range(BW + 1):
            lhs, rhs = [low], [keep_if(strict_up, own) if t == 0 else w[BW + r, t]]
            for m in range(1, BW + 1 - t):
                lhs.append(l[r, BW - m])
                rhs.append(w[BW + r - m, t + m])
            value = w0[BW + r, t].astype(F32) - mm(lhs, rhs)
            if t == 0:
                value = jnp.where(strict_low, value * pivot, value)
            else:
                keep = msg[pl.ds(rows + r, 1), :] >= float(t)
                value = jnp.where(jnp.broadcast_to(keep, (size, size)), value, 0.0)
            w_new[new_row, t] = value.astype(BF16)

    def lower_row(r, w, l, l_new):
        for k in range(BW):
            m = BW - k
            lhs, rhs = [l[r, k]], [keep_if(strict_up, w[BW + r - m, 0])]
            for back in range(m + 1, BW + 1):
                lhs.append(l[r, BW - back])
                rhs.append(w[BW + r - back, back - m])
            value = (l0[r, k].astype(F32) - mm(lhs, rhs)) * rd[pl.ds(BW + r - m, 1), :]
            keep = reach[pl.ds(r, 1), :] >= float(m)
            l_new[r, k] = jnp.where(jnp.broadcast_to(keep, (size, size)), value, 0.0).astype(BF16)

    def arrive(r, pieces, when):
        for c in range(rows):
            if pieces[c]:

                @pl.when(jnp.logical_and(when, r == c))
                def _():
                    for piece in pieces[c]:
                        piece.wait_recv()

    relayed = [[on_copy(j, False) for j in range(n_plain) if by_relay[j][0] == r] for r in range(rows)]
    relayed_edge = [[on_copy(j, True) for j in range(rows, n_edge) if by_relay_edge[j][0] == r] for r in range(rows)]
    relayed_base = [[on_copy(rows - 1 - r, True)] for r in range(rows)]
    direct_rest = [[x_rest(from_first, 0, BW - DIRECT, BW)] if r == 0 else [] for r in range(rows)]
    direct_rest_edge = [[x_rest(from_first, 0, 0, BW)] if r == 0 else [] for r in range(rows)]
    beside_rest = [[x_rest(from_first, r, 0, BW - r)] for r in range(rows)]
    x_first = [[x_crit(from_first, r, BW + 1)] for r in range(rows)]
    x_first_edge = [[x_crit(from_first, r, BW)] if r else [] for r in range(rows)]
    y_first = [[y_part(w1.at[BW + r], r, 0)] if r else [] for r in range(rows)]
    y_rest = [
        [y_part(w1.at[BW + r], r, kind) for kind in ((1, 2, 3) if r < rows - 1 else (2, 3))] for r in range(rows)
    ]

    @pl.when(edge_in)
    def _():
        for copy in g_copies:
            copy.wait_recv()

    def last_column(r, diag_block, old):
        keep = above[pl.ds(rows + r, 1), :] >= float(BW)
        value = base[r].astype(F32) - mm([keep_if(strict_low, diag_block)], [old])
        return jnp.where(jnp.broadcast_to(keep, (size, size)), value, 0.0).astype(BF16)

    def upper_1(i, c):
        r = rows - 1 - i
        arrive(r, x_first, grp > 0)
        arrive(r, x_first_edge, edge_in)
        arrive(r, relayed_base, edge_in)

        @pl.when(grp > 0)
        def _():
            lax.fori_loop(BW - r, BW + 1, above_upper(r), 0)
            base[r] = w0[r, BW]

        @pl.when(grp == 0)
        def _():
            keep = above[pl.ds(rows + r, 1), :] >= float(BW)
            base[r] = scaled(base[r], r, r + BW, keep)
            first_diag = scaled_diag(diag0[r], r, above[pl.ds(r, 1), :])
            w0[r, BW] = last_column(r, first_diag, base[r])

        upper_row(r, w0, l0, w1, BW + r)
        return c

    @pl.when(jnp.logical_not(has_prev))
    def _():
        def clear(a, c):
            base[a] = jnp.zeros((size, size), BF16)
            diag0[a] = jnp.zeros((size, size), BF16)
            return c

        lax.fori_loop(0, rows, clear, 0)

    lax.fori_loop(0, rows, upper_1, 0)

    @pl.when(jnp.logical_not(odd))
    def _():
        for part in y_parts(lambda r: w1.at[BW + r]):
            part.start()

    @pl.when(edge_out)
    def _():
        for r in range(rows - 1, 0, -1):
            x_crit(from_first, r, BW).start()
        for j in range(rows, n_edge):
            out_copy(j, True).start()
        x_rest(from_first, 0, 0, BW).start()

    def lower_1(i, c):
        r = rows - 1 - i
        arrive(r, beside_rest, odd)
        plain = jnp.logical_and(from_relay, grp > 0)
        arrive(r, relayed, plain)
        arrive(r, direct_rest, plain)
        arrive(r, relayed_edge, edge_in)
        arrive(r, direct_rest_edge, edge_in)

        @pl.when(grp > 0)
        def _():
            w0[r, 0] = scaled_diag(w0[r, 0], r, above[pl.ds(r, 1), :])
            lax.fori_loop(1, BW - r, above_upper(r), 0)

        rd[pl.ds(r, 1), :] = 1.0 / diagonal(w0[r, 0])
        lower_row(r, w0, l0, l1)
        return c

    lax.fori_loop(0, rows, lower_1, 0)

    half_way = n_edge // 2
    forward(range(half_way))

    @pl.when(inside_odd)
    def _():
        for part in y_parts(lambda r: w1.at[BW + r]):
            part.start()


    @pl.when(grp < n_grp - 1)
    def _():
        forward(range(half_way, n_edge))

    def upper_2(i, c):
        r = rows - 1 - i
        arrive(r, y_first, has_prev)
        w1[r, BW] = last_column(r, w0[r, 0], w0[r, BW])
        upper_row(r, w1, l1, wo, r)
        return c

    lax.fori_loop(0, rows, upper_2, 0)

    @pl.when(edge_out)
    def _():
        for part in y_parts(lambda r: wo.at[r]):
            part.start()

    @pl.when(grp == n_grp - 1)
    def _():
        forward(range(half_way, n_edge))

    def lower_2(i, c):
        r = rows - 1 - i
        arrive(r, y_rest, has_prev)
        rd[pl.ds(r, 1), :] = 1.0 / diagonal(w1[r, 0])
        lower_row(r, w1, l1, lo)
        return c

    lax.fori_loop(0, rows, lower_2, 0)

    @pl.when(has_next)
    def _():
        for part in y_parts(lambda r: w1.at[BW + r]) + [to_next]:
            part.wait_send()

    @pl.when(inside)
    def _():
        for r in downward:
            x_crit(from_first, r, BW + 1).wait_send()

    @pl.when(jnp.logical_not(odd))
    def _():
        for r in downward:
            x_rest(from_first, r, 0, BW - r).wait_send()

    @pl.when(inside_odd)
    def _():
        for j in range(n_plain):
            out_copy(j, False).wait_send()
        x_rest(from_first, 0, BW - DIRECT, BW).wait_send()

    @pl.when(edge_out)
    def _():
        for copy in g_copies:
            copy.wait_send()
        for r in range(rows - 1, 0, -1):
            x_crit(from_first, r, BW).wait_send()
        for j in range(n_edge):
            out_copy(j, True).wait_send()
        x_rest(from_first, 0, 0, BW).wait_send()

    @pl.when(relaying_plain)
    def _():
        for j in range(n_plain):
            on_copy(j, False).wait_send()

    @pl.when(origin_edge)
    def _():
        for j in range(n_edge):
            on_copy(j, True).wait_send()

    @pl.when(has_prev)
    def _():
        to_prev.wait_send()


def per_device(n_slab, n_grp, blocks, diag_shift, offsets):
    rows, band, size, _ = blocks.shape
    block = (size, size)
    n_rest = BW * (BW + 1) // 2
    call = pl.pallas_call(
        functools.partial(kernel, n_slab, n_grp),
        out_shape=pltpu.VMEM(blocks.shape, BF16),
        in_specs=[
            pl.BlockSpec(memory_space=pltpu.HBM),
            pl.BlockSpec(memory_space=pltpu.HBM),
            pl.BlockSpec(memory_space=pltpu.HBM),
        ],
        out_specs=pl.BlockSpec(memory_space=pltpu.VMEM),
        scratch_shapes=[
            pltpu.VMEM((2 * rows, BW + 1) + block, BF16),
            pltpu.VMEM((rows, BW) + block, BF16),
            pltpu.VMEM((2 * rows, BW + 1) + block, BF16),
            pltpu.VMEM((rows, BW) + block, BF16),
            pltpu.VMEM((rows,) + block, BF16),
            pltpu.VMEM((rows,) + block, BF16),
            pltpu.VMEM((n_rest,) + block, BF16),
            pltpu.VMEM((rows * size,), F32),
            pltpu.VMEM((2, rows), jnp.int32),
            pltpu.VMEM((2 * rows, size), F32),
            pltpu.VMEM((2 * rows, size), F32),
            pltpu.VMEM((2 * rows, size), F32),
            pltpu.VMEM((2 * rows, size), F32),
            pltpu.VMEM((4 * rows, size), F32),
            pltpu.VMEM((2 * rows, size, LANES), F32),
            pltpu.VMEM((2 * rows, size), F32),
            pltpu.SemaphoreType.DMA((5,)),
            pltpu.SemaphoreType.DMA((2,)),
            pltpu.SemaphoreType.DMA((2,)),
            pltpu.SemaphoreType.DMA((2 * rows,)),
            pltpu.SemaphoreType.DMA((2 * rows,)),
            pltpu.SemaphoreType.DMA((4 * rows,)),
            pltpu.SemaphoreType.DMA((4 * rows,)),
            pltpu.SemaphoreType.DMA((2,)),
            pltpu.SemaphoreType.DMA((2,)),
        ] + [pltpu.SemaphoreType.DMA((n_rest,))] * 4,
        compiler_params=pltpu.CompilerParams(
            collective_id=0, has_side_effects=True, vmem_limit_bytes=67_043_328 - 2 * blocks.size
        ),
        name="sweeps",
    )
    return call(blocks, diag_shift, offsets.T)


def solution(mesh):
    return jax.shard_map(
        functools.partial(per_device, mesh.shape["slab"], mesh.shape["grp"]),
        mesh=mesh,
        in_specs=(
            P(("slab", "grp"), None, None, None),
            P(("slab", "grp")),
            P(("slab", "grp"), None),
        ),
        out_specs=P(("slab", "grp"), None, None, None),
        check_vma=False,
    )
```

```python
import functools

import jax
import jax.numpy as jnp
from jax import lax
from jax.experimental import pallas as pl
from jax.experimental.pallas import tpu as pltpu
from jax.sharding import PartitionSpec as P

MESH = pl.DeviceIdType.MESH
F32 = jnp.float32
BF16 = jnp.bfloat16
BW = 4
LANES = 128
DIRECT = 2
DIRECT_EDGE = 1


def mm(lhs, rhs):
    lhs = lhs[0] if len(lhs) == 1 else jnp.concatenate(lhs, axis=1)
    rhs = rhs[0] if len(rhs) == 1 else jnp.concatenate(rhs, axis=0)
    return jnp.dot(lhs, rhs, preferred_element_type=F32)


def kernel(
    n_slab, n_grp,
    blocks, shift_in, offs_in, out,
    w0, l0, w1, l1,
    base, diag0, relay, packed, corner, corner_in, shift, offs, msg, above, below, reach, sc, rs, rd,
    in_sem, m_send, m_recv, x_send, x_recv, y_send, y_recv, g_send, g_recv,
    o_send, o_recv, r_send, r_recv,
):
    rows, _, size, _ = blocks.shape
    wo, lo = out.at[:, pl.ds(BW, BW + 1)], out.at[:, pl.ds(0, BW)]
    half = size // 2
    slab, grp = lax.axis_index("slab"), lax.axis_index("grp")
    flat = slab * n_grp + grp
    total = n_slab * n_grp
    has_prev, has_next = flat > 0, flat < total - 1
    after, before = jnp.minimum(flat + 1, total - 1), jnp.maximum(flat - 1, 0)
    nxt = (after // n_grp, after % n_grp)
    prv = (before // n_grp, before % n_grp)

    n_x, n_zh = n_slab // 2, min(4, n_grp // 2)
    odd = grp % 2 == 1

    def along_z(place, step):
        slab_at, grp_at = place
        z = (grp_at // 2 % n_zh * 2 + slab_at // n_x + step + 4 * n_zh) % (2 * n_zh)
        return (z % 2 * n_x + slab_at % n_x, grp_at // (2 * n_zh) * (2 * n_zh) + z // 2 * 2 + grp_at % 2)

    my_relay = along_z((slab, grp), -3)
    origin = along_z((slab, grp), 3)
    prv_relay = along_z(prv, -3)
    origin_flat = origin[0] * n_grp + origin[1]
    target_flat = jnp.minimum(origin_flat + 1, total - 1)
    target = (target_flat // n_grp, target_flat % n_grp)
    relaying = jnp.logical_and(odd, origin_flat < total - 1)
    origin_edge = jnp.logical_and(relaying, origin[1] == n_grp - 1)
    inside = grp < n_grp - 1
    edge_out = jnp.logical_and(has_next, grp == n_grp - 1)
    edge_in = jnp.logical_and(has_prev, grp == 0)

    def remote(src, dst, send, recv, where_to):
        return pltpu.make_async_remote_copy(
            src_ref=src, dst_ref=dst, send_sem=send, recv_sem=recv, device_id=where_to, device_id_type=MESH
        )

    loads = [
        pltpu.make_async_copy(blocks.at[:, BW], w0.at[pl.ds(BW, rows), 0], in_sem.at[0]),
        pltpu.make_async_copy(blocks.at[:, pl.ds(BW + 1, BW)], w0.at[pl.ds(BW, rows), pl.ds(1, BW)], in_sem.at[1]),
        pltpu.make_async_copy(blocks.at[:, pl.ds(0, BW)], l0, in_sem.at[2]),
        pltpu.make_async_copy(shift_in, shift, in_sem.at[3]),
        pltpu.make_async_copy(offs_in, offs, in_sem.at[4]),
    ]
    for load in loads:
        load.start()

    barrier = pltpu.get_barrier_semaphore()

    @pl.when(has_next)
    def _():
        pl.semaphore_signal(barrier, inc=1, device_id=nxt, device_id_type=MESH)

    @pl.when(has_prev)
    def _():
        pl.semaphore_signal(barrier, inc=1, device_id=prv, device_id_type=MESH)

    @pl.when(odd)
    def _():
        pl.semaphore_signal(barrier, inc=1, device_id=origin, device_id_type=MESH)

    from_relay = jnp.logical_and(has_prev, jnp.logical_not(odd))

    @pl.when(from_relay)
    def _():
        pl.semaphore_signal(barrier, inc=1, device_id=prv_relay, device_id_type=MESH)

    one = jnp.int32(1)
    peers = sum(jnp.where(c, one, 0) for c in (has_next, has_prev, odd, relaying))
    pl.semaphore_wait(barrier, peers)

    def x_crit(source, r, last):
        first = BW - r
        cut = pl.ds(first, last - first)
        return remote(source(r, first, last - first), w0.at[r, cut], x_send.at[r], x_recv.at[r], nxt)

    def x_rest(source, r, first, last):
        cut = pl.ds(first, last - first)
        at = rows + r
        return remote(source(r, first, last - first), w0.at[r, cut], x_send.at[at], x_recv.at[at], nxt)

    def from_input(r, first, count):
        return blocks.at[r, pl.ds(BW + first, count)]

    def from_first(r, first, count):
        return w1.at[BW + r, pl.ds(first, count)]

    downward = list(range(rows - 1, -1, -1))
    rest = [(r, t) for r in downward for t in range(BW - r)]
    n_plain, n_edge = len(rest) - DIRECT, len(rest) - DIRECT_EDGE

    def out_copy(j, source=from_first):
        r, t = rest[j]
        return remote(source(r, t, 1), relay.at[pl.ds(j, 1)], o_send.at[j], o_recv.at[j], my_relay)

    def on_copy(j):
        r, t = rest[j]
        return remote(relay.at[pl.ds(j, 1)], w0.at[r, pl.ds(t, 1)], r_send.at[j], r_recv.at[j], target)

    relaying_plain = jnp.logical_and(relaying, jnp.logical_not(origin_edge))

    def forward(js):
        for j in js:

            @pl.when(relaying_plain if j >= n_edge else origin_edge if j >= n_plain else relaying)
            def _():
                out_copy(j).wait_recv()
                on_copy(j).start()

    def y_part(row_ref, r, kind):
        at = r * 3 + kind
        sems = (y_send.at[at], y_recv.at[at], nxt)
        if kind == 2:
            return remote(packed.at[r], w1.at[r, 0, pl.ds(0, half)], *sems)
        cut = pl.ds(1, BW - 1 - r) if kind else pl.ds(BW - r, r)
        return remote(row_ref.at[cut], w1.at[r, cut], *sems)

    corner_copy = remote(corner, corner_in, y_send.at[3 * rows], y_recv.at[3 * rows], nxt)

    def y_parts(source):
        order = [(r, 0) for r in range(rows - 1, 0, -1)]
        for r in range(rows - 1, -1, -1):
            order += [(r, 1)] * (r < rows - 1) + [(r, 2)]
        return [corner_copy] + [y_part(source(r), r, kind) for r, kind in order]

    inside_odd = jnp.logical_and(inside, odd)
    half_rows = pl.ds(half, half)
    g_copies = [
        remote(blocks.at[:, 2 * BW], base, g_send.at[2], g_recv.at[2], nxt),
        remote(blocks.at[:, BW, half_rows], diag0.at[:, half_rows], g_send.at[0], g_recv.at[0], nxt),
        remote(
            blocks.at[:, BW, pl.ds(0, half), pl.ds(0, half)],
            diag0.at[:, pl.ds(0, half), pl.ds(0, half)],
            g_send.at[1], g_recv.at[1], nxt,
        ),
    ]

    @pl.when(inside_odd)
    def _():
        for j in range(n_plain):
            out_copy(j, from_input).start()

    @pl.when(jnp.logical_not(has_prev))
    def _():
        above[...] = jnp.zeros_like(above)

        def clear(i, c):
            a, t = i // (BW + 1), i % (BW + 1)
            w0[a, t] = jnp.zeros((size, size), BF16)
            w1[a, t] = jnp.zeros((size, size), BF16)
            return c

        lax.fori_loop(0, BW * (BW + 1), clear, 0)

    @pl.when(jnp.logical_not(has_next))
    def _():
        below[...] = jnp.zeros_like(below)

    row_id = lax.broadcasted_iota(jnp.int32, (size, size), 0)
    col_id = lax.broadcasted_iota(jnp.int32, (size, size), 1)
    eye = row_id == col_id

    def diagonal(block):
        return jnp.sum(jnp.where(eye, block.astype(F32), 0.0), axis=0, keepdims=True)

    loads[0].wait()
    loads[3].wait()
    loads[4].wait()
    reaches = offs[...]
    for r in range(rows):
        msg[pl.ds(r, 1), :] = shift[pl.ds(r * size, size)].reshape(1, size) + diagonal(w0[BW + r, 0])
        at = flat * rows + r
        up = jnp.minimum(reaches[1:2, r : r + 1], total * rows - 1 - at)
        down = jnp.minimum(reaches[0:1, r : r + 1], at)
        msg[pl.ds(rows + r, 1), :] = jnp.broadcast_to(up.astype(F32), (1, size))
        reach[pl.ds(r, 1), :] = jnp.broadcast_to(down.astype(F32), (1, size))
    to_next = remote(msg, above, m_send.at[0], m_recv.at[0], nxt)
    to_prev = remote(msg, below, m_send.at[1], m_recv.at[1], prv)

    @pl.when(has_next)
    def _():
        to_next.start()

    @pl.when(has_prev)
    def _():
        to_prev.start()

    @pl.when(inside)
    def _():
        for r in downward:
            x_crit(from_input, r, BW + 1).start()

    @pl.when(jnp.logical_not(odd))
    def _():
        for r in downward:
            x_rest(from_input, r, 0, BW - r).start()

    @pl.when(edge_out)
    def _():
        for copy in g_copies:
            copy.start()

    loads[1].wait()
    loads[2].wait()

    @pl.when(has_prev)
    def _():
        to_next.wait_recv()

    @pl.when(has_next)
    def _():
        to_prev.wait_recv()

    def scale_of(values):
        positive = values > 0
        return jnp.where(positive, 1.0 / jnp.sqrt(jnp.where(positive, values, 1.0)), 0.0)

    sc[pl.ds(0, rows), :] = scale_of(above[pl.ds(0, rows), :])
    sc[pl.ds(rows, rows), :] = scale_of(msg[pl.ds(0, rows), :])
    sc[pl.ds(2 * rows, rows), :] = scale_of(below[pl.ds(0, rows), :])

    def spread(j, c):
        column = jnp.sum(jnp.where(eye, jnp.broadcast_to(sc[pl.ds(j, 1), :], (size, size)), 0.0), axis=1, keepdims=True)
        rs[j] = jnp.broadcast_to(column, (size, LANES))
        return c

    lax.fori_loop(0, 2 * rows, spread, 0)

    def scaled(block, j, column, keep):
        row_scale = jnp.concatenate([rs[j]] * (size // LANES), axis=1)
        value = block.astype(F32) * row_scale * sc[pl.ds(column, 1), :]
        return jnp.where(jnp.broadcast_to(keep, (size, size)), value, 0.0).astype(BF16)

    def scaled_diag(block, j, values):
        row_scale = jnp.concatenate([rs[j]] * (size // LANES), axis=1)
        full = jnp.where(eye, jnp.broadcast_to(values, (size, size)), block.astype(F32))
        return (full * row_scale * sc[pl.ds(j, 1), :]).astype(BF16)

    def own_upper(i, c):
        r, t = i // BW, 1 + i % BW
        keep = msg[pl.ds(rows + r, 1), :] >= t.astype(F32)
        w0[BW + r, t] = scaled(w0[BW + r, t], BW + r, BW + r + t, keep)
        return c

    def own_lower(i, c):
        r, k = i // BW, i % BW
        keep = reach[pl.ds(r, 1), :] >= (BW - k).astype(F32)
        l0[r, k] = scaled(l0[r, k], BW + r, r + k, keep)
        return c

    def own_diag(r, c):
        w0[BW + r, 0] = scaled_diag(w0[BW + r, 0], BW + r, msg[pl.ds(r, 1), :])
        rd[pl.ds(BW + r, 1), :] = 1.0 / diagonal(w0[BW + r, 0])
        return c

    lax.fori_loop(0, rows, own_diag, 0)
    lax.fori_loop(0, rows * BW, own_upper, 0)
    lax.fori_loop(0, rows * BW, own_lower, 0)

    def above_upper(a):
        def step(t, c):
            keep = above[pl.ds(rows + a, 1), :] >= t.astype(F32)
            w0[a, t] = scaled(w0[a, t], a, a + t, keep)
            return c

        return step

    strict_up, strict_low = col_id > row_id, row_id > col_id

    def keep_if(mask, block):
        return jnp.where(mask, block.astype(F32), 0.0).astype(BF16)

    again = 2 * rows

    def upper_row(r, w, l, w_new, new_row, at):
        own = w[BW + r, 0]
        low = keep_if(strict_low, own)
        pivot = rd[pl.ds(at + BW + r, 1), :]
        for t in range(BW + 1):
            lhs, rhs = [low], [keep_if(strict_up, own) if t == 0 else w[BW + r, t]]
            for m in range(1, BW + 1 - t):
                lhs.append(l[r, BW - m])
                rhs.append(w[BW + r - m, t + m])
            value = w0[BW + r, t].astype(F32) - mm(lhs, rhs)
            if t == 0:
                value = jnp.where(strict_low, value * pivot, value)
            else:
                keep = msg[pl.ds(rows + r, 1), :] >= float(t)
                value = jnp.where(jnp.broadcast_to(keep, (size, size)), value, 0.0)
            w_new[new_row, t] = value.astype(BF16)

    row_half = lax.broadcasted_iota(jnp.int32, (half, half), 0)
    col_half = lax.broadcasted_iota(jnp.int32, (half, half), 1)
    eye_half = row_half == col_half
    low_half, high_half = pl.ds(0, half), pl.ds(half, half)

    def pack(r, w, row):
        last = w[row, 0, high_half, high_half].astype(F32)
        first = jnp.where(col_half >= row_half, w[row, 0, low_half, low_half].astype(F32), last.T)
        packed[r, :, low_half] = first.astype(BF16)
        packed[r, :, high_half] = w[row, 0, low_half, high_half]
        corner[pl.ds(r, 1), :] = jnp.sum(jnp.where(eye_half, last, 0.0), axis=0, keepdims=True)

    def unpack(r):
        first = w1[r, 0, low_half, low_half].astype(F32)
        values = jnp.broadcast_to(corner_in[pl.ds(r, 1), :], (half, half))
        last = jnp.where(col_half > row_half, first.T, jnp.where(eye_half, values, 0.0))
        w1[r, 0, high_half, high_half] = last.astype(BF16)

    def lower_row(r, w, l, l_new, at):
        for k in range(BW):
            m = BW - k
            lhs, rhs = [l[r, k]], [keep_if(strict_up, w[BW + r - m, 0])]
            for back in range(m + 1, BW + 1):
                lhs.append(l[r, BW - back])
                rhs.append(w[BW + r - back, back - m])
            value = (l0[r, k].astype(F32) - mm(lhs, rhs)) * rd[pl.ds(at + BW + r - m, 1), :]
            keep = reach[pl.ds(r, 1), :] >= float(m)
            l_new[r, k] = jnp.where(jnp.broadcast_to(keep, (size, size)), value, 0.0).astype(BF16)

    def arrive(r, pieces, when):
        for c in range(rows):
            if pieces[c]:

                @pl.when(jnp.logical_and(when, r == c))
                def _():
                    for piece in pieces[c]:
                        piece.wait_recv()

    def by_row(js):
        return [[on_copy(j) for j in js if rest[j][0] == r] for r in range(rows)]

    relayed, relayed_edge = by_row(range(n_plain)), by_row(range(n_edge))
    direct_rest = [[x_rest(from_first, 0, BW - DIRECT, BW)] if r == 0 and DIRECT else [] for r in range(rows)]
    direct_rest_edge = [
        [x_rest(from_first, 0, BW - DIRECT_EDGE, BW)] if r == 0 and DIRECT_EDGE else [] for r in range(rows)
    ]
    beside_rest = [[x_rest(from_first, r, 0, BW - r)] for r in range(rows)]
    x_first = [[x_crit(from_first, r, BW + 1)] for r in range(rows)]
    x_first_edge = [[x_crit(from_first, r, BW)] if r else [] for r in range(rows)]
    y_first = [[y_part(w1.at[BW + r], r, 0)] if r else [] for r in range(rows)]
    y_rest = [[y_part(w1.at[BW + r], r, kind) for kind in ((1, 2) if r < rows - 1 else (2,))] for r in range(rows)]
    y_rest[rows - 1].append(corner_copy)

    @pl.when(edge_in)
    def _():
        for copy in g_copies:
            copy.wait_recv()

    def last_column(r, diag_block, old):
        keep = above[pl.ds(rows + r, 1), :] >= float(BW)
        value = base[r].astype(F32) - mm([keep_if(strict_low, diag_block)], [old])
        return jnp.where(jnp.broadcast_to(keep, (size, size)), value, 0.0).astype(BF16)

    def upper_1(i, c):
        r = rows - 1 - i
        arrive(r, x_first, grp > 0)
        arrive(r, x_first_edge, edge_in)

        @pl.when(grp > 0)
        def _():
            lax.fori_loop(BW - r, BW + 1, above_upper(r), 0)
            base[r] = w0[r, BW]

        @pl.when(grp == 0)
        def _():
            keep = above[pl.ds(rows + r, 1), :] >= float(BW)
            base[r] = scaled(base[r], r, r + BW, keep)
            first_diag = scaled_diag(diag0[r], r, above[pl.ds(r, 1), :])
            w0[r, BW] = last_column(r, first_diag, base[r])

        upper_row(r, w0, l0, w1, BW + r, 0)
        rd[pl.ds(again + BW + r, 1), :] = 1.0 / diagonal(w1[BW + r, 0])
        pack(r, w1, BW + r)
        return c

    @pl.when(jnp.logical_not(has_prev))
    def _():
        def clear(a, c):
            base[a] = jnp.zeros((size, size), BF16)
            diag0[a] = jnp.zeros((size, size), BF16)
            return c

        lax.fori_loop(0, rows, clear, 0)

    lax.fori_loop(0, rows, upper_1, 0)

    @pl.when(jnp.logical_not(odd))
    def _():
        for part in y_parts(lambda r: w1.at[BW + r]):
            part.start()

    @pl.when(edge_out)
    def _():
        for r in range(rows - 1, 0, -1):
            x_crit(from_first, r, BW).start()
        for j in range(n_edge):
            out_copy(j).start()
        if DIRECT_EDGE:
            x_rest(from_first, 0, BW - DIRECT_EDGE, BW).start()

    def lower_1(i, c):
        r = rows - 1 - i
        arrive(r, beside_rest, odd)
        plain = jnp.logical_and(from_relay, grp > 0)
        arrive(r, relayed, plain)
        arrive(r, direct_rest, plain)
        arrive(r, relayed_edge, edge_in)
        arrive(r, direct_rest_edge, edge_in)

        @pl.when(grp > 0)
        def _():
            w0[r, 0] = scaled_diag(w0[r, 0], r, above[pl.ds(r, 1), :])
            lax.fori_loop(1, BW - r, above_upper(r), 0)

        rd[pl.ds(r, 1), :] = 1.0 / diagonal(w0[r, 0])
        lower_row(r, w0, l0, l1, 0)
        return c

    @pl.when(odd)
    def _():
        lax.fori_loop(0, rows, lower_1, 0)

    n_most = max(n_plain, n_edge)
    half_way = n_most // 2
    forward(range(half_way))

    @pl.when(inside_odd)
    def _():
        x_rest(from_input, 0, BW - DIRECT, BW).start()
        for part in y_parts(lambda r: w1.at[BW + r]):
            part.start()


    @pl.when(grp < n_grp - 1)
    def _():
        forward(range(half_way, n_most))

    def upper_2(i, c):
        r = rows - 1 - i
        arrive(r, y_first, has_prev)
        w1[r, BW] = last_column(r, w0[r, 0], w0[r, BW])
        upper_row(r, w1, l1, wo, r, again)

        @pl.when(edge_out)
        def _():
            pack(r, wo, r)

        return c

    def lower_2(i, c):
        r = rows - 1 - i
        arrive(r, y_rest, has_prev)

        @pl.when(has_prev)
        def _():
            unpack(r)

        rd[pl.ds(again + r, 1), :] = 1.0 / diagonal(w1[r, 0])
        lower_row(r, w1, l1, lo, again)
        return c

    @pl.when(odd)
    def _():
        lax.fori_loop(0, rows, upper_2, 0)

    @pl.when(edge_out)
    def _():
        for part in y_parts(lambda r: wo.at[r]):
            part.start()

    @pl.when(grp == n_grp - 1)
    def _():
        forward(range(half_way, n_most))

    def finish(i, c):
        @pl.when(jnp.logical_not(odd))
        def _():
            lower_1(i, c)
            upper_2(i, c)

        lower_2(i, c)
        return c

    lax.fori_loop(0, rows, finish, 0)

    @pl.when(has_next)
    def _():
        for part in y_parts(lambda r: w1.at[BW + r]) + [to_next]:
            part.wait_send()

    @pl.when(inside)
    def _():
        for r in downward:
            x_crit(from_first, r, BW + 1).wait_send()

    @pl.when(jnp.logical_not(odd))
    def _():
        for r in downward:
            x_rest(from_first, r, 0, BW - r).wait_send()

    @pl.when(inside_odd)
    def _():
        for j in range(n_plain):
            out_copy(j).wait_send()
        x_rest(from_first, 0, BW - DIRECT, BW).wait_send()

    @pl.when(edge_out)
    def _():
        for copy in g_copies:
            copy.wait_send()
        for r in range(rows - 1, 0, -1):
            x_crit(from_first, r, BW).wait_send()
        for j in range(n_edge):
            out_copy(j).wait_send()
        if DIRECT_EDGE:
            x_rest(from_first, 0, BW - DIRECT_EDGE, BW).wait_send()

    @pl.when(relaying_plain)
    def _():
        for j in range(n_plain):
            on_copy(j).wait_send()

    @pl.when(origin_edge)
    def _():
        for j in range(n_edge):
            on_copy(j).wait_send()

    @pl.when(has_prev)
    def _():
        to_prev.wait_send()


def per_device(n_slab, n_grp, blocks, diag_shift, offsets):
    rows, band, size, _ = blocks.shape
    block = (size, size)
    n_rest = BW * (BW + 1) // 2
    call = pl.pallas_call(
        functools.partial(kernel, n_slab, n_grp),
        out_shape=pltpu.VMEM(blocks.shape, BF16),
        in_specs=[
            pl.BlockSpec(memory_space=pltpu.HBM),
            pl.BlockSpec(memory_space=pltpu.HBM),
            pl.BlockSpec(memory_space=pltpu.HBM),
        ],
        out_specs=pl.BlockSpec(memory_space=pltpu.VMEM),
        scratch_shapes=[
            pltpu.VMEM((2 * rows, BW + 1) + block, BF16),
            pltpu.VMEM((rows, BW) + block, BF16),
            pltpu.VMEM((2 * rows, BW + 1) + block, BF16),
            pltpu.VMEM((rows, BW) + block, BF16),
            pltpu.VMEM((rows,) + block, BF16),
            pltpu.VMEM((rows,) + block, BF16),
            pltpu.VMEM((n_rest,) + block, BF16),
            pltpu.VMEM((rows, size // 2, size), BF16),
            pltpu.VMEM((2 * rows, size // 2), F32),
            pltpu.VMEM((2 * rows, size // 2), F32),
            pltpu.VMEM((rows * size,), F32),
            pltpu.VMEM((2, rows), jnp.int32),
            pltpu.VMEM((2 * rows, size), F32),
            pltpu.VMEM((2 * rows, size), F32),
            pltpu.VMEM((2 * rows, size), F32),
            pltpu.VMEM((2 * rows, size), F32),
            pltpu.VMEM((4 * rows, size), F32),
            pltpu.VMEM((2 * rows, size, LANES), F32),
            pltpu.VMEM((4 * rows, size), F32),
            pltpu.SemaphoreType.DMA((5,)),
            pltpu.SemaphoreType.DMA((2,)),
            pltpu.SemaphoreType.DMA((2,)),
            pltpu.SemaphoreType.DMA((2 * rows,)),
            pltpu.SemaphoreType.DMA((2 * rows,)),
            pltpu.SemaphoreType.DMA((4 * rows,)),
            pltpu.SemaphoreType.DMA((4 * rows,)),
            pltpu.SemaphoreType.DMA((3,)),
            pltpu.SemaphoreType.DMA((3,)),
        ] + [pltpu.SemaphoreType.DMA((n_rest,))] * 4,
        compiler_params=pltpu.CompilerParams(
            collective_id=0, has_side_effects=True, vmem_limit_bytes=67_043_328 - 2 * blocks.size
        ),
        name="sweeps",
    )
    return call(blocks, diag_shift, offsets.T)


def solution(mesh):
    return jax.shard_map(
        functools.partial(per_device, mesh.shape["slab"], mesh.shape["grp"]),
        mesh=mesh,
        in_specs=(
            P(("slab", "grp"), None, None, None),
            P(("slab", "grp")),
            P(("slab", "grp"), None),
        ),
        out_specs=P(("slab", "grp"), None, None, None),
        check_vma=False,
    )
```

```python
import functools

import jax
import jax.numpy as jnp
from jax import lax
from jax.experimental import pallas as pl
from jax.experimental.pallas import tpu as pltpu
from jax.sharding import PartitionSpec as P

MESH = pl.DeviceIdType.MESH
F32 = jnp.float32
BF16 = jnp.bfloat16
BW = 4
LANES = 128
DIRECT = 2
DIRECT_EDGE = 3
HEAD = 2
CHIPS_ZH = 4


def mm(lhs, rhs):
    lhs = lhs[0] if len(lhs) == 1 else jnp.concatenate(lhs, axis=1)
    rhs = rhs[0] if len(rhs) == 1 else jnp.concatenate(rhs, axis=0)
    return jnp.dot(lhs, rhs, preferred_element_type=F32)


def kernel(
    n_slab, n_grp,
    blocks, shift_in, offs_in, out,
    w0, l0, w1, l1,
    base, diag0, packed0, side_block, relay, packed, corner, corner_in, shift, offs, msg, above, below, reach, sc, rs, rd,
    in_sem, m_send, m_recv, x_send, x_recv, y_send, y_recv, g_send, g_recv,
    o_send, o_recv, r_send, r_recv, s_send, s_recv, t_send, t_recv,
):
    rows, _, size, _ = blocks.shape
    wo, lo = out.at[:, pl.ds(BW, BW + 1)], out.at[:, pl.ds(0, BW)]
    half = size // 2
    slab, grp = lax.axis_index("slab"), lax.axis_index("grp")
    flat = slab * n_grp + grp
    total = n_slab * n_grp
    has_prev, has_next = flat > 0, flat < total - 1
    after, before = jnp.minimum(flat + 1, total - 1), jnp.maximum(flat - 1, 0)
    nxt = (after // n_grp, after % n_grp)
    prv = (before // n_grp, before % n_grp)

    n_x, n_zh = n_slab // 2, min(CHIPS_ZH, n_grp // 2)
    odd = grp % 2 == 1

    def along_z(place, step):
        slab_at, grp_at = place
        z = (grp_at // 2 % n_zh * 2 + slab_at // n_x + step + 4 * n_zh) % (2 * n_zh)
        return (z % 2 * n_x + slab_at % n_x, grp_at // (2 * n_zh) * (2 * n_zh) + z // 2 * 2 + grp_at % 2)

    def relay_of(place):
        slab_at, grp_at = along_z(place, -3)
        return (slab_at, jnp.where(grp_at == n_grp - 1, n_grp - 2, grp_at))

    my_relay, prv_relay = relay_of((slab, grp)), relay_of(prv)
    is_relay = jnp.logical_or(jnp.logical_and(odd, grp != n_grp - 1), grp == n_grp - 2)
    origin = along_z((slab, grp // 2 * 2 + 1), 3)
    origin_flat = origin[0] * n_grp + origin[1]
    target_flat = jnp.minimum(origin_flat + 1, total - 1)
    target = (target_flat // n_grp, target_flat % n_grp)
    relaying = jnp.logical_and(is_relay, origin_flat < total - 1)
    origin_edge = jnp.logical_and(relaying, origin[1] == n_grp - 1)

    n_side = n_grp // (2 * n_zh) - 1
    side_back = (n_grp - 2 - grp) // (2 * n_zh)
    on_side = jnp.logical_and(slab < n_slab - 1, (n_grp - 2 - grp) % (2 * n_zh) == 0)
    on_side = jnp.logical_and(on_side, side_back > 0)
    edge_after, edge_last = (jnp.minimum(slab + 1, n_slab - 1), 0), (slab, n_grp - 1)

    def side(slab_at, k):
        return (slab_at, n_grp - 2 - 2 * n_zh * k)
    inside = grp < n_grp - 1
    edge_out = jnp.logical_and(has_next, grp == n_grp - 1)
    edge_in = jnp.logical_and(has_prev, grp == 0)

    def remote(src, dst, send, recv, where_to):
        return pltpu.make_async_remote_copy(
            src_ref=src, dst_ref=dst, send_sem=send, recv_sem=recv, device_id=where_to, device_id_type=MESH
        )

    loads = [
        pltpu.make_async_copy(blocks.at[:, BW], w0.at[pl.ds(BW, rows), 0], in_sem.at[0]),
        pltpu.make_async_copy(blocks.at[:, pl.ds(BW + 1, BW)], w0.at[pl.ds(BW, rows), pl.ds(1, BW)], in_sem.at[1]),
        pltpu.make_async_copy(blocks.at[:, pl.ds(0, BW)], l0, in_sem.at[2]),
        pltpu.make_async_copy(shift_in, shift, in_sem.at[3]),
        pltpu.make_async_copy(offs_in, offs, in_sem.at[4]),
    ]
    for load in loads:
        load.start()

    barrier = pltpu.get_barrier_semaphore()

    @pl.when(has_next)
    def _():
        pl.semaphore_signal(barrier, inc=1, device_id=nxt, device_id_type=MESH)

    @pl.when(has_prev)
    def _():
        pl.semaphore_signal(barrier, inc=1, device_id=prv, device_id_type=MESH)

    @pl.when(is_relay)
    def _():
        pl.semaphore_signal(barrier, inc=1, device_id=origin, device_id_type=MESH)

    from_relay = jnp.logical_and(has_prev, jnp.logical_not(odd))

    @pl.when(from_relay)
    def _():
        pl.semaphore_signal(barrier, inc=1, device_id=prv_relay, device_id_type=MESH)

    @pl.when(on_side)
    def _():
        pl.semaphore_signal(barrier, inc=1, device_id=edge_last, device_id_type=MESH)

    @pl.when(edge_in)
    def _():
        for k in range(1, n_side + 1):
            pl.semaphore_signal(barrier, inc=1, device_id=side(prv[0], k), device_id_type=MESH)

    one = jnp.int32(1)
    peers = sum(jnp.where(c, one, 0) for c in (has_next, has_prev, odd, relaying, on_side))
    peers = peers + jnp.where(edge_out, jnp.int32(n_side), 0)
    pl.semaphore_wait(barrier, peers)

    def x_crit(source, r, last):
        first = BW - r
        cut = pl.ds(first, last - first)
        return remote(source(r, first, last - first), w0.at[r, cut], x_send.at[r], x_recv.at[r], nxt)

    def x_rest(source, r, first, last):
        cut = pl.ds(first, last - first)
        at = rows + r
        return remote(source(r, first, last - first), w0.at[r, cut], x_send.at[at], x_recv.at[at], nxt)

    def from_input(r, first, count):
        return blocks.at[r, pl.ds(BW + first, count)]

    def from_first(r, first, count):
        return w1.at[BW + r, pl.ds(first, count)]

    downward = list(range(rows - 1, -1, -1))
    rest = [(r, t) for r in downward for t in range(BW - r)]
    n_plain, n_edge = len(rest) - DIRECT, len(rest) - DIRECT_EDGE
    inside_odd = jnp.logical_and(inside, odd)

    def out_copy(j, source=from_first):
        r, t = rest[j]
        return remote(source(r, t, 1), relay.at[pl.ds(j, 1)], o_send.at[j], o_recv.at[j], my_relay)

    def on_copy(j):
        r, t = rest[j]
        return remote(relay.at[pl.ds(j, 1)], w0.at[r, pl.ds(t, 1)], r_send.at[j], r_recv.at[j], target)

    relays_plain = jnp.logical_and(relaying, jnp.logical_not(origin_edge))
    by_kind = ((relays_plain, n_plain), (origin_edge, n_edge))

    def forward(js):
        for j in js:

            mine = jnp.bool_(False)
            for kind, count in by_kind:
                mine = jnp.logical_or(mine, jnp.logical_and(kind, j < count))

            @pl.when(mine)
            def _():
                out_copy(j).wait_recv()
                on_copy(j).start()

    def y_part(row_ref, r, kind):
        at = r * 3 + kind
        sems = (y_send.at[at], y_recv.at[at], nxt)
        if kind == 2:
            return remote(packed.at[r], w1.at[r, 0, pl.ds(0, half)], *sems)
        cut = pl.ds(1, BW - 1 - r) if kind else pl.ds(BW - r, r)
        return remote(row_ref.at[cut], w1.at[r, cut], *sems)

    corner_copy = remote(corner, corner_in, y_send.at[3 * rows], y_recv.at[3 * rows], nxt)

    def side_out(k):
        return remote(wo.at[0, k], side_block.at[0], s_send.at[k - 1], s_recv.at[k - 1], side(slab, k))

    def side_on(k):
        return remote(side_block.at[0], w1.at[0, k], t_send.at[k - 1], t_recv.at[k - 1], edge_after)

    def y_edge():
        cut = pl.ds(1 + n_side, BW - 1 - n_side)
        return [remote(wo.at[0, cut], w1.at[0, cut], y_send.at[1], y_recv.at[1], nxt)] if BW - 1 > n_side else []

    def y_parts_edge():
        order = [(r, 0) for r in range(rows - 1, 0, -1)]
        for r in range(rows - 1, 0, -1):
            order += [(r, 1)] * (r < rows - 1) + [(r, 2)]
        parts = [y_part(wo.at[r], r, kind) for r, kind in order]
        return [corner_copy] + parts + y_edge() + [y_part(wo.at[0], 0, 2)]

    def y_parts(source):
        order = [(r, 0) for r in range(rows - 1, 0, -1)]
        for r in range(rows - 1, -1, -1):
            order += [(r, 1)] * (r < rows - 1) + [(r, 2)]
        return [corner_copy] + [y_part(source(r), r, kind) for r, kind in order]

    g_copies = [
        remote(blocks.at[:, 2 * BW], base, g_send.at[0], g_recv.at[0], nxt),
        remote(packed0, diag0, g_send.at[1], g_recv.at[1], nxt),
    ]

    @pl.when(inside_odd)
    def _():
        for j in range(n_plain):
            out_copy(j, from_input).start()

    head = downward[rows - HEAD :]

    @pl.when(inside_odd)
    def _():
        for r in head:
            x_crit(from_input, r, BW + 1).start()

    @pl.when(edge_out)
    def _():
        g_copies[0].start()

    @pl.when(jnp.logical_not(has_prev))
    def _():
        above[...] = jnp.zeros_like(above)

        def clear(i, c):
            a, t = i // (BW + 1), i % (BW + 1)
            w0[a, t] = jnp.zeros((size, size), BF16)
            w1[a, t] = jnp.zeros((size, size), BF16)
            return c

        lax.fori_loop(0, BW * (BW + 1), clear, 0)

    @pl.when(jnp.logical_not(has_next))
    def _():
        below[...] = jnp.zeros_like(below)

    row_id = lax.broadcasted_iota(jnp.int32, (size, size), 0)
    col_id = lax.broadcasted_iota(jnp.int32, (size, size), 1)
    eye = row_id == col_id

    row_half = lax.broadcasted_iota(jnp.int32, (half, half), 0)
    col_half = lax.broadcasted_iota(jnp.int32, (half, half), 1)
    eye_half = row_half == col_half
    low_half, high_half = pl.ds(0, half), pl.ds(half, half)

    def diagonal(block):
        return jnp.sum(jnp.where(eye, block.astype(F32), 0.0), axis=0, keepdims=True)

    loads[0].wait()
    loads[3].wait()
    loads[4].wait()
    reaches = offs[...]
    for r in range(rows):
        msg[pl.ds(r, 1), :] = shift[pl.ds(r * size, size)].reshape(1, size) + diagonal(w0[BW + r, 0])
        at = flat * rows + r
        up = jnp.minimum(reaches[1:2, r : r + 1], total * rows - 1 - at)
        down = jnp.minimum(reaches[0:1, r : r + 1], at)
        msg[pl.ds(rows + r, 1), :] = jnp.broadcast_to(up.astype(F32), (1, size))
        reach[pl.ds(r, 1), :] = jnp.broadcast_to(down.astype(F32), (1, size))
    to_next = remote(msg, above, m_send.at[0], m_recv.at[0], nxt)
    to_prev = remote(msg, below, m_send.at[1], m_recv.at[1], prv)

    @pl.when(has_next)
    def _():
        to_next.start()

    @pl.when(has_prev)
    def _():
        to_prev.start()

    @pl.when(inside)
    def _():
        for r in downward[: rows - HEAD]:
            x_crit(from_input, r, BW + 1).start()

    @pl.when(jnp.logical_not(odd))
    def _():
        for r in head:
            x_crit(from_input, r, BW + 1).start()

    @pl.when(jnp.logical_not(odd))
    def _():
        for r in downward:
            x_rest(from_input, r, 0, BW - r).start()

    @pl.when(edge_out)
    def _():
        def pack_low(r, c):
            first = w0[BW + r, 0, low_half, low_half].astype(F32)
            last = w0[BW + r, 0, high_half, high_half].astype(F32)
            packed0[r, :, low_half] = jnp.where(col_half < row_half, first, last.T).astype(BF16)
            packed0[r, :, high_half] = w0[BW + r, 0, high_half, low_half]
            return c

        lax.fori_loop(0, rows, pack_low, 0)
        g_copies[1].start()

    loads[1].wait()
    loads[2].wait()

    @pl.when(has_prev)
    def _():
        to_next.wait_recv()

    @pl.when(has_next)
    def _():
        to_prev.wait_recv()

    def scale_of(values):
        positive = values > 0
        return jnp.where(positive, 1.0 / jnp.sqrt(jnp.where(positive, values, 1.0)), 0.0)

    sc[pl.ds(0, rows), :] = scale_of(above[pl.ds(0, rows), :])
    sc[pl.ds(rows, rows), :] = scale_of(msg[pl.ds(0, rows), :])
    sc[pl.ds(2 * rows, rows), :] = scale_of(below[pl.ds(0, rows), :])

    def spread(j, c):
        column = jnp.sum(jnp.where(eye, jnp.broadcast_to(sc[pl.ds(j, 1), :], (size, size)), 0.0), axis=1, keepdims=True)
        rs[j] = jnp.broadcast_to(column, (size, LANES))
        return c

    lax.fori_loop(0, 2 * rows, spread, 0)

    def scaled(block, j, column, keep):
        row_scale = jnp.concatenate([rs[j]] * (size // LANES), axis=1)
        value = block.astype(F32) * row_scale * sc[pl.ds(column, 1), :]
        return jnp.where(jnp.broadcast_to(keep, (size, size)), value, 0.0).astype(BF16)

    def scaled_diag(block, j, values):
        row_scale = jnp.concatenate([rs[j]] * (size // LANES), axis=1)
        full = jnp.where(eye, jnp.broadcast_to(values, (size, size)), block.astype(F32))
        return (full * row_scale * sc[pl.ds(j, 1), :]).astype(BF16)

    def own_upper(i, c):
        r, t = i // BW, 1 + i % BW
        keep = msg[pl.ds(rows + r, 1), :] >= t.astype(F32)
        w0[BW + r, t] = scaled(w0[BW + r, t], BW + r, BW + r + t, keep)
        return c

    def own_lower(i, c):
        r, k = i // BW, i % BW
        keep = reach[pl.ds(r, 1), :] >= (BW - k).astype(F32)
        l0[r, k] = scaled(l0[r, k], BW + r, r + k, keep)
        return c

    def own_diag(r, c):
        w0[BW + r, 0] = scaled_diag(w0[BW + r, 0], BW + r, msg[pl.ds(r, 1), :])
        rd[pl.ds(BW + r, 1), :] = 1.0 / diagonal(w0[BW + r, 0])
        return c

    lax.fori_loop(0, rows, own_diag, 0)
    lax.fori_loop(0, rows * BW, own_upper, 0)
    lax.fori_loop(0, rows * BW, own_lower, 0)

    def above_upper(a):
        def step(t, c):
            keep = above[pl.ds(rows + a, 1), :] >= t.astype(F32)
            w0[a, t] = scaled(w0[a, t], a, a + t, keep)
            return c

        return step

    strict_up, strict_low = col_id > row_id, row_id > col_id

    def keep_if(mask, block):
        return jnp.where(mask, block.astype(F32), 0.0).astype(BF16)

    again = 2 * rows

    def upper_row(r, w, l, w_new, new_row, at):
        own = w[BW + r, 0]
        low = keep_if(strict_low, own)
        pivot = rd[pl.ds(at + BW + r, 1), :]
        for t in range(BW + 1):
            lhs, rhs = [low], [keep_if(strict_up, own) if t == 0 else w[BW + r, t]]
            for m in range(1, BW + 1 - t):
                lhs.append(l[r, BW - m])
                rhs.append(w[BW + r - m, t + m])
            value = w0[BW + r, t].astype(F32) - mm(lhs, rhs)
            if t == 0:
                value = jnp.where(strict_low, value * pivot, value)
            else:
                keep = msg[pl.ds(rows + r, 1), :] >= float(t)
                value = jnp.where(jnp.broadcast_to(keep, (size, size)), value, 0.0)
            w_new[new_row, t] = value.astype(BF16)

    def pack(r, w, row):
        last = w[row, 0, high_half, high_half].astype(F32)
        first = jnp.where(col_half >= row_half, w[row, 0, low_half, low_half].astype(F32), last.T)
        packed[r, :, low_half] = first.astype(BF16)
        packed[r, :, high_half] = w[row, 0, low_half, high_half]
        corner[pl.ds(r, 1), :] = jnp.sum(jnp.where(eye_half, last, 0.0), axis=0, keepdims=True)

    def unpack(r):
        first = w1[r, 0, low_half, low_half].astype(F32)
        values = jnp.broadcast_to(corner_in[pl.ds(r, 1), :], (half, half))
        last = jnp.where(col_half > row_half, first.T, jnp.where(eye_half, values, 0.0))
        w1[r, 0, high_half, high_half] = last.astype(BF16)

    def lower_row(r, w, l, l_new, at):
        for k in range(BW):
            m = BW - k
            lhs, rhs = [l[r, k]], [keep_if(strict_up, w[BW + r - m, 0])]
            for back in range(m + 1, BW + 1):
                lhs.append(l[r, BW - back])
                rhs.append(w[BW + r - back, back - m])
            value = (l0[r, k].astype(F32) - mm(lhs, rhs)) * rd[pl.ds(at + BW + r - m, 1), :]
            keep = reach[pl.ds(r, 1), :] >= float(m)
            l_new[r, k] = jnp.where(jnp.broadcast_to(keep, (size, size)), value, 0.0).astype(BF16)

    def arrive(r, pieces, when):
        for c in range(rows):
            if pieces[c]:

                @pl.when(jnp.logical_and(when, r == c))
                def _():
                    for piece in pieces[c]:
                        piece.wait_recv()

    def by_row(js):
        return [[on_copy(j) for j in js if rest[j][0] == r] for r in range(rows)]

    def rest_kind(count):
        by_link = by_row(range(len(rest) - count))
        by_link[0].append(x_rest(from_first, 0, BW - count, BW))
        return by_link

    rest_kinds = (
        (jnp.logical_and(from_relay, grp > 0), rest_kind(DIRECT)),
        (edge_in, rest_kind(DIRECT_EDGE)),
    )
    beside_rest = [[x_rest(from_first, r, 0, BW - r)] for r in range(rows)]
    x_first = [[x_crit(from_first, r, BW + 1)] for r in range(rows)]
    x_first_edge = [[x_crit(from_first, r, BW)] if r else [] for r in range(rows)]
    y_first = [[y_part(w1.at[BW + r], r, 0)] if r else [] for r in range(rows)]
    y_rest = [[y_part(w1.at[BW + r], r, kind) for kind in ((1, 2) if r < rows - 1 else (2,))] for r in range(rows)]
    y_rest[rows - 1].append(corner_copy)
    y_last, y_rest[0] = y_rest[0], []
    y_last_edge = y_edge() + [y_part(w1.at[BW], 0, 2)] + [side_on(k) for k in range(1, n_side + 1)]

    @pl.when(edge_in)
    def _():
        for copy in g_copies:
            copy.wait_recv()

    def last_column(r, diag_block, old):
        keep = above[pl.ds(rows + r, 1), :] >= float(BW)
        value = base[r].astype(F32) - mm([keep_if(strict_low, diag_block)], [old])
        return jnp.where(jnp.broadcast_to(keep, (size, size)), value, 0.0).astype(BF16)

    def upper_1(i, c):
        r = rows - 1 - i
        arrive(r, x_first, grp > 0)
        arrive(r, x_first_edge, edge_in)

        @pl.when(grp > 0)
        def _():
            lax.fori_loop(BW - r, BW + 1, above_upper(r), 0)
            base[r] = w0[r, BW]

        @pl.when(grp == 0)
        def _():
            keep = above[pl.ds(rows + r, 1), :] >= float(BW)
            base[r] = scaled(base[r], r, r + BW, keep)
            first = diag0[r, :, low_half].astype(F32)
            top = jnp.concatenate([first, jnp.zeros((half, half), F32)], axis=1)
            bottom = jnp.concatenate([diag0[r, :, high_half].astype(F32), first.T], axis=1)
            first_diag = scaled_diag(jnp.concatenate([top, bottom], axis=0), r, above[pl.ds(r, 1), :])
            w0[r, BW] = last_column(r, first_diag, base[r])

        upper_row(r, w0, l0, w1, BW + r, 0)
        rd[pl.ds(again + BW + r, 1), :] = 1.0 / diagonal(w1[BW + r, 0])
        pack(r, w1, BW + r)
        return c

    @pl.when(jnp.logical_not(has_prev))
    def _():
        def clear(a, c):
            base[a] = jnp.zeros((size, size), BF16)
            diag0[a] = jnp.zeros((half, size), BF16)
            return c

        lax.fori_loop(0, rows, clear, 0)

    lax.fori_loop(0, rows, upper_1, 0)

    @pl.when(jnp.logical_not(odd))
    def _():
        for part in y_parts(lambda r: w1.at[BW + r]):
            part.start()

    @pl.when(edge_out)
    def _():
        for r in range(rows - 1, 0, -1):
            x_crit(from_first, r, BW).start()
        for j in range(n_edge):
            out_copy(j).start()
        x_rest(from_first, 0, BW - DIRECT_EDGE, BW).start()

    def lower_1(i, c):
        r = rows - 1 - i
        arrive(r, beside_rest, odd)
        for kind, pieces in rest_kinds:
            arrive(r, pieces, kind)

        @pl.when(grp > 0)
        def _():
            w0[r, 0] = scaled_diag(w0[r, 0], r, above[pl.ds(r, 1), :])
            lax.fori_loop(1, BW - r, above_upper(r), 0)

        rd[pl.ds(r, 1), :] = 1.0 / diagonal(w0[r, 0])
        lower_row(r, w0, l0, l1, 0)
        return c

    @pl.when(odd)
    def _():
        lax.fori_loop(0, rows, lower_1, 0)

    n_most = max(n_plain, n_edge)
    half_way = n_most // 2
    forward(range(half_way))

    @pl.when(inside_odd)
    def _():
        x_rest(from_input, 0, BW - DIRECT, BW).start()
        for part in y_parts(lambda r: w1.at[BW + r]):
            part.start()

    forward(range(half_way, n_most))

    def upper_2(i, c):
        r = rows - 1 - i
        arrive(r, y_first, has_prev)
        w1[r, BW] = last_column(r, w0[r, 0], w0[r, BW])
        upper_row(r, w1, l1, wo, r, again)

        @pl.when(edge_out)
        def _():
            pack(r, wo, r)

        return c

    def lower_2(i, c):
        r = rows - 1 - i
        arrive(r, y_rest, has_prev)
        arrive(r, [y_last] + [[]] * (rows - 1), grp > 0)
        arrive(r, [y_last_edge] + [[]] * (rows - 1), edge_in)

        @pl.when(has_prev)
        def _():
            unpack(r)

        rd[pl.ds(again + r, 1), :] = 1.0 / diagonal(w1[r, 0])
        lower_row(r, w1, l1, lo, again)
        return c

    for k in range(1, n_side + 1):

        @pl.when(jnp.logical_and(on_side, side_back == k))
        def _():
            side_out(k).wait_recv()
            side_on(k).start()

    @pl.when(odd)
    def _():
        lax.fori_loop(0, rows, upper_2, 0)

    @pl.when(edge_out)
    def _():
        for k in range(1, n_side + 1):
            side_out(k).start()
        for part in y_parts_edge():
            part.start()

    def finish(i, c):
        @pl.when(jnp.logical_not(odd))
        def _():
            lower_1(i, c)
            upper_2(i, c)

        lower_2(i, c)
        return c

    lax.fori_loop(0, rows, finish, 0)

    @pl.when(has_next)
    def _():
        to_next.wait_send()

    for k in range(1, n_side + 1):

        @pl.when(jnp.logical_and(on_side, side_back == k))
        def _():
            side_on(k).wait_send()

    @pl.when(inside)
    def _():
        for part in y_parts(lambda r: w1.at[BW + r]):
            part.wait_send()
        for r in downward:
            x_crit(from_first, r, BW + 1).wait_send()

    @pl.when(jnp.logical_not(odd))
    def _():
        for r in downward:
            x_rest(from_first, r, 0, BW - r).wait_send()

    @pl.when(inside_odd)
    def _():
        for j in range(n_plain):
            out_copy(j).wait_send()
        x_rest(from_first, 0, BW - DIRECT, BW).wait_send()

    @pl.when(edge_out)
    def _():
        for k in range(1, n_side + 1):
            side_out(k).wait_send()
        for part in y_parts_edge():
            part.wait_send()
        for copy in g_copies:
            copy.wait_send()
        for r in range(rows - 1, 0, -1):
            x_crit(from_first, r, BW).wait_send()
        for j in range(n_edge):
            out_copy(j).wait_send()
        x_rest(from_first, 0, BW - DIRECT_EDGE, BW).wait_send()

    for kind, count in by_kind:

        @pl.when(kind)
        def _():
            for j in range(count):
                on_copy(j).wait_send()

    @pl.when(has_prev)
    def _():
        to_prev.wait_send()


def per_device(n_slab, n_grp, blocks, diag_shift, offsets):
    rows, band, size, _ = blocks.shape
    block = (size, size)
    n_rest = BW * (BW + 1) // 2
    call = pl.pallas_call(
        functools.partial(kernel, n_slab, n_grp),
        out_shape=pltpu.VMEM(blocks.shape, BF16),
        in_specs=[
            pl.BlockSpec(memory_space=pltpu.HBM),
            pl.BlockSpec(memory_space=pltpu.HBM),
            pl.BlockSpec(memory_space=pltpu.HBM),
        ],
        out_specs=pl.BlockSpec(memory_space=pltpu.VMEM),
        scratch_shapes=[
            pltpu.VMEM((2 * rows, BW + 1) + block, BF16),
            pltpu.VMEM((rows, BW) + block, BF16),
            pltpu.VMEM((2 * rows, BW + 1) + block, BF16),
            pltpu.VMEM((rows, BW) + block, BF16),
            pltpu.VMEM((rows,) + block, BF16),
            pltpu.VMEM((rows, size // 2, size), BF16),
            pltpu.VMEM((rows, size // 2, size), BF16),
            pltpu.VMEM((1,) + block, BF16),
            pltpu.VMEM((n_rest,) + block, BF16),
            pltpu.VMEM((rows, size // 2, size), BF16),
            pltpu.VMEM((2 * rows, size // 2), F32),
            pltpu.VMEM((2 * rows, size // 2), F32),
            pltpu.VMEM((rows * size,), F32),
            pltpu.VMEM((2, rows), jnp.int32),
            pltpu.VMEM((2 * rows, size), F32),
            pltpu.VMEM((2 * rows, size), F32),
            pltpu.VMEM((2 * rows, size), F32),
            pltpu.VMEM((2 * rows, size), F32),
            pltpu.VMEM((4 * rows, size), F32),
            pltpu.VMEM((2 * rows, size, LANES), F32),
            pltpu.VMEM((4 * rows, size), F32),
            pltpu.SemaphoreType.DMA((5,)),
            pltpu.SemaphoreType.DMA((2,)),
            pltpu.SemaphoreType.DMA((2,)),
            pltpu.SemaphoreType.DMA((2 * rows,)),
            pltpu.SemaphoreType.DMA((2 * rows,)),
            pltpu.SemaphoreType.DMA((4 * rows,)),
            pltpu.SemaphoreType.DMA((4 * rows,)),
            pltpu.SemaphoreType.DMA((3,)),
            pltpu.SemaphoreType.DMA((3,)),
        ] + [pltpu.SemaphoreType.DMA((n_rest,))] * 4 + [pltpu.SemaphoreType.DMA((rows,))] * 4,
        compiler_params=pltpu.CompilerParams(
            collective_id=0, has_side_effects=True, vmem_limit_bytes=67_043_328 - 2 * blocks.size
        ),
        name="sweeps",
    )
    return call(blocks, diag_shift, offsets.T)


def solution(mesh):
    return jax.shard_map(
        functools.partial(per_device, mesh.shape["slab"], mesh.shape["grp"]),
        mesh=mesh,
        in_specs=(
            P(("slab", "grp"), None, None, None),
            P(("slab", "grp")),
            P(("slab", "grp"), None),
        ),
        out_specs=P(("slab", "grp"), None, None, None),
        check_vma=False,
    )
```

```python
import functools

import jax
import jax.numpy as jnp
from jax import lax
from jax.experimental import pallas as pl
from jax.experimental.pallas import tpu as pltpu
from jax.sharding import PartitionSpec as P

MESH = pl.DeviceIdType.MESH
F32 = jnp.float32
BF16 = jnp.bfloat16
BW = 4
LANES = 128
DIRECT = 2
DIRECT_EDGE = 3
HEAD = 1
CHIPS_ZH = 4


def mm(lhs, rhs):
    lhs = lhs[0] if len(lhs) == 1 else jnp.concatenate(lhs, axis=1)
    rhs = rhs[0] if len(rhs) == 1 else jnp.concatenate(rhs, axis=0)
    return jnp.dot(lhs, rhs, preferred_element_type=F32)


def kernel(
    n_slab, n_grp,
    blocks, shift_in, offs_in, out,
    w0, l0, w1, l1,
    base, diag0, packed0, side_block, relay, packed, corner, corner_in, shift, offs, msg, above, below, reach, sc, rs, rd,
    in_sem, m_send, m_recv, x_send, x_recv, y_send, y_recv, g_send, g_recv,
    o_send, o_recv, r_send, r_recv, s_send, s_recv, t_send, t_recv,
):
    rows, _, size, _ = blocks.shape
    wo, lo = out.at[:, pl.ds(BW, BW + 1)], out.at[:, pl.ds(0, BW)]
    half = size // 2
    slab, grp = lax.axis_index("slab"), lax.axis_index("grp")
    flat = slab * n_grp + grp
    total = n_slab * n_grp
    has_prev, has_next = flat > 0, flat < total - 1
    after, before = jnp.minimum(flat + 1, total - 1), jnp.maximum(flat - 1, 0)
    nxt = (after // n_grp, after % n_grp)
    prv = (before // n_grp, before % n_grp)

    n_x, n_zh = n_slab // 2, min(CHIPS_ZH, n_grp // 2)
    odd = grp % 2 == 1

    def along_z(place, step):
        slab_at, grp_at = place
        z = (grp_at // 2 % n_zh * 2 + slab_at // n_x + step + 4 * n_zh) % (2 * n_zh)
        return (z % 2 * n_x + slab_at % n_x, grp_at // (2 * n_zh) * (2 * n_zh) + z // 2 * 2 + grp_at % 2)

    def relay_of(place):
        slab_at, grp_at = along_z(place, -3)
        return (slab_at, jnp.where(grp_at == n_grp - 1, n_grp - 2, grp_at))

    my_relay, prv_relay = relay_of((slab, grp)), relay_of(prv)
    is_relay = jnp.logical_or(jnp.logical_and(odd, grp != n_grp - 1), grp == n_grp - 2)
    origin = along_z((slab, grp // 2 * 2 + 1), 3)
    origin_flat = origin[0] * n_grp + origin[1]
    target_flat = jnp.minimum(origin_flat + 1, total - 1)
    target = (target_flat // n_grp, target_flat % n_grp)
    relaying = jnp.logical_and(is_relay, origin_flat < total - 1)
    origin_edge = jnp.logical_and(relaying, origin[1] == n_grp - 1)

    n_side = n_grp // (2 * n_zh) - 1
    side_back = (n_grp - 2 - grp) // (2 * n_zh)
    on_side = jnp.logical_and(slab < n_slab - 1, (n_grp - 2 - grp) % (2 * n_zh) == 0)
    on_side = jnp.logical_and(on_side, side_back > 0)
    edge_after, edge_last = (jnp.minimum(slab + 1, n_slab - 1), 0), (slab, n_grp - 1)

    def side(slab_at, k):
        return (slab_at, n_grp - 2 - 2 * n_zh * k)
    inside = grp < n_grp - 1
    edge_out = jnp.logical_and(has_next, grp == n_grp - 1)
    edge_in = jnp.logical_and(has_prev, grp == 0)

    def remote(src, dst, send, recv, where_to):
        return pltpu.make_async_remote_copy(
            src_ref=src, dst_ref=dst, send_sem=send, recv_sem=recv, device_id=where_to, device_id_type=MESH
        )

    loads = [
        pltpu.make_async_copy(blocks.at[:, BW], w0.at[pl.ds(BW, rows), 0], in_sem.at[0]),
        pltpu.make_async_copy(blocks.at[:, pl.ds(BW + 1, BW)], w0.at[pl.ds(BW, rows), pl.ds(1, BW)], in_sem.at[1]),
        pltpu.make_async_copy(blocks.at[:, pl.ds(0, BW)], l0, in_sem.at[2]),
        pltpu.make_async_copy(shift_in, shift, in_sem.at[3]),
        pltpu.make_async_copy(offs_in, offs, in_sem.at[4]),
    ]
    for load in loads:
        load.start()

    barrier = pltpu.get_barrier_semaphore()

    @pl.when(has_next)
    def _():
        pl.semaphore_signal(barrier, inc=1, device_id=nxt, device_id_type=MESH)

    @pl.when(has_prev)
    def _():
        pl.semaphore_signal(barrier, inc=1, device_id=prv, device_id_type=MESH)

    @pl.when(is_relay)
    def _():
        pl.semaphore_signal(barrier, inc=1, device_id=origin, device_id_type=MESH)

    from_relay = jnp.logical_and(has_prev, jnp.logical_not(odd))

    @pl.when(from_relay)
    def _():
        pl.semaphore_signal(barrier, inc=1, device_id=prv_relay, device_id_type=MESH)

    @pl.when(on_side)
    def _():
        pl.semaphore_signal(barrier, inc=1, device_id=edge_last, device_id_type=MESH)

    @pl.when(edge_in)
    def _():
        for k in range(1, n_side + 1):
            pl.semaphore_signal(barrier, inc=1, device_id=side(prv[0], k), device_id_type=MESH)

    one = jnp.int32(1)
    peers = sum(jnp.where(c, one, 0) for c in (has_next, has_prev, odd, relaying, on_side))
    peers = peers + jnp.where(edge_out, jnp.int32(n_side), 0)
    pl.semaphore_wait(barrier, peers)

    def x_crit(source, r, last):
        first = BW - r
        cut = pl.ds(first, last - first)
        return remote(source(r, first, last - first), w0.at[r, cut], x_send.at[r], x_recv.at[r], nxt)

    def x_rest(source, r, first, last):
        cut = pl.ds(first, last - first)
        at = rows + r
        return remote(source(r, first, last - first), w0.at[r, cut], x_send.at[at], x_recv.at[at], nxt)

    def from_input(r, first, count):
        return blocks.at[r, pl.ds(BW + first, count)]

    def from_first(r, first, count):
        return w1.at[BW + r, pl.ds(first, count)]

    downward = list(range(rows - 1, -1, -1))
    rest = [(r, t) for r in downward for t in range(BW - r)]
    n_plain, n_edge = len(rest) - DIRECT, len(rest) - DIRECT_EDGE
    inside_odd = jnp.logical_and(inside, odd)

    def out_copy(j, source=from_first):
        r, t = rest[j]
        return remote(source(r, t, 1), relay.at[pl.ds(j, 1)], o_send.at[j], o_recv.at[j], my_relay)

    def on_copy(j):
        r, t = rest[j]
        return remote(relay.at[pl.ds(j, 1)], w0.at[r, pl.ds(t, 1)], r_send.at[j], r_recv.at[j], target)

    relays_plain = jnp.logical_and(relaying, jnp.logical_not(origin_edge))
    by_kind = ((relays_plain, n_plain), (origin_edge, n_edge))

    def forward(js):
        for j in js:

            mine = jnp.bool_(False)
            for kind, count in by_kind:
                mine = jnp.logical_or(mine, jnp.logical_and(kind, j < count))

            @pl.when(mine)
            def _():
                out_copy(j).wait_recv()
                on_copy(j).start()

    def y_part(row_ref, r, kind):
        at = r * 3 + kind
        sems = (y_send.at[at], y_recv.at[at], nxt)
        if kind == 2:
            return remote(packed.at[r], w1.at[r, 0, pl.ds(0, half)], *sems)
        cut = pl.ds(1, BW - 1 - r) if kind else pl.ds(BW - r, r)
        return remote(row_ref.at[cut], w1.at[r, cut], *sems)

    corner_copy = remote(corner, corner_in, y_send.at[3 * rows], y_recv.at[3 * rows], nxt)

    def side_out(k):
        return remote(wo.at[0, k], side_block.at[0], s_send.at[k - 1], s_recv.at[k - 1], side(slab, k))

    def side_on(k):
        return remote(side_block.at[0], w1.at[0, k], t_send.at[k - 1], t_recv.at[k - 1], edge_after)

    def y_edge():
        cut = pl.ds(1 + n_side, BW - 1 - n_side)
        return [remote(wo.at[0, cut], w1.at[0, cut], y_send.at[1], y_recv.at[1], nxt)] if BW - 1 > n_side else []

    def y_parts_edge():
        order = [(r, 0) for r in range(rows - 1, 0, -1)]
        for r in range(rows - 1, 0, -1):
            order += [(r, 1)] * (r < rows - 1) + [(r, 2)]
        parts = [y_part(wo.at[r], r, kind) for r, kind in order]
        return [corner_copy] + parts + y_edge() + [y_part(wo.at[0], 0, 2)]

    def y_parts(source):
        order = [(r, 0) for r in range(rows - 1, 0, -1)]
        for r in range(rows - 1, -1, -1):
            order += [(r, 1)] * (r < rows - 1) + [(r, 2)]
        return [corner_copy] + [y_part(source(r), r, kind) for r, kind in order]

    g_copies = [
        remote(blocks.at[:, 2 * BW], base, g_send.at[0], g_recv.at[0], nxt),
        remote(packed0, diag0, g_send.at[1], g_recv.at[1], nxt),
    ]

    @pl.when(inside_odd)
    def _():
        for j in range(n_plain):
            out_copy(j, from_input).start()

    head = downward[rows - HEAD :]

    @pl.when(inside_odd)
    def _():
        for r in head:
            x_crit(from_input, r, BW + 1).start()

    @pl.when(edge_out)
    def _():
        g_copies[0].start()

    @pl.when(jnp.logical_not(has_prev))
    def _():
        above[...] = jnp.zeros_like(above)

        def clear(i, c):
            a, t = i // (BW + 1), i % (BW + 1)
            w0[a, t] = jnp.zeros((size, size), BF16)
            w1[a, t] = jnp.zeros((size, size), BF16)
            return c

        lax.fori_loop(0, BW * (BW + 1), clear, 0)

    @pl.when(jnp.logical_not(has_next))
    def _():
        below[...] = jnp.zeros_like(below)

    row_id = lax.broadcasted_iota(jnp.int32, (size, size), 0)
    col_id = lax.broadcasted_iota(jnp.int32, (size, size), 1)
    eye = row_id == col_id

    row_half = lax.broadcasted_iota(jnp.int32, (half, half), 0)
    col_half = lax.broadcasted_iota(jnp.int32, (half, half), 1)
    eye_half = row_half == col_half
    low_half, high_half = pl.ds(0, half), pl.ds(half, half)

    def diagonal(block):
        return jnp.sum(jnp.where(eye, block.astype(F32), 0.0), axis=0, keepdims=True)

    loads[0].wait()
    loads[3].wait()
    loads[4].wait()
    reaches = offs[...]
    for r in range(rows):
        msg[pl.ds(r, 1), :] = shift[pl.ds(r * size, size)].reshape(1, size) + diagonal(w0[BW + r, 0])
        at = flat * rows + r
        up = jnp.minimum(reaches[1:2, r : r + 1], total * rows - 1 - at)
        down = jnp.minimum(reaches[0:1, r : r + 1], at)
        msg[pl.ds(rows + r, 1), :] = jnp.broadcast_to(up.astype(F32), (1, size))
        reach[pl.ds(r, 1), :] = jnp.broadcast_to(down.astype(F32), (1, size))
    to_next = remote(msg, above, m_send.at[0], m_recv.at[0], nxt)
    to_prev = remote(msg, below, m_send.at[1], m_recv.at[1], prv)

    @pl.when(has_next)
    def _():
        to_next.start()

    @pl.when(has_prev)
    def _():
        to_prev.start()

    @pl.when(inside)
    def _():
        for r in downward[: rows - HEAD]:
            x_crit(from_input, r, BW + 1).start()

    @pl.when(jnp.logical_not(odd))
    def _():
        for r in head:
            x_crit(from_input, r, BW + 1).start()

    @pl.when(jnp.logical_not(odd))
    def _():
        for r in downward:
            x_rest(from_input, r, 0, BW - r).start()

    @pl.when(edge_out)
    def _():
        def pack_low(r, c):
            first = w0[BW + r, 0, low_half, low_half].astype(F32)
            last = w0[BW + r, 0, high_half, high_half].astype(F32)
            packed0[r, :, low_half] = jnp.where(col_half < row_half, first, last.T).astype(BF16)
            packed0[r, :, high_half] = w0[BW + r, 0, high_half, low_half]
            return c

        lax.fori_loop(0, rows, pack_low, 0)
        g_copies[1].start()

    loads[1].wait()
    loads[2].wait()

    @pl.when(has_prev)
    def _():
        to_next.wait_recv()

    @pl.when(has_next)
    def _():
        to_prev.wait_recv()

    def scale_of(values):
        positive = values > 0
        return jnp.where(positive, 1.0 / jnp.sqrt(jnp.where(positive, values, 1.0)), 0.0)

    sc[pl.ds(0, rows), :] = scale_of(above[pl.ds(0, rows), :])
    sc[pl.ds(rows, rows), :] = scale_of(msg[pl.ds(0, rows), :])
    sc[pl.ds(2 * rows, rows), :] = scale_of(below[pl.ds(0, rows), :])

    def spread(j, c):
        column = jnp.sum(jnp.where(eye, jnp.broadcast_to(sc[pl.ds(j, 1), :], (size, size)), 0.0), axis=1, keepdims=True)
        rs[j] = jnp.broadcast_to(column, (size, LANES))
        return c

    lax.fori_loop(0, 2 * rows, spread, 0)

    def scaled(block, j, column, keep):
        row_scale = jnp.concatenate([rs[j]] * (size // LANES), axis=1)
        value = block.astype(F32) * row_scale * sc[pl.ds(column, 1), :]
        return jnp.where(jnp.broadcast_to(keep, (size, size)), value, 0.0).astype(BF16)

    def scaled_diag(block, j, values):
        row_scale = jnp.concatenate([rs[j]] * (size // LANES), axis=1)
        full = jnp.where(eye, jnp.broadcast_to(values, (size, size)), block.astype(F32))
        return (full * row_scale * sc[pl.ds(j, 1), :]).astype(BF16)

    def own_upper(i, c):
        r, t = i // BW, 1 + i % BW
        keep = msg[pl.ds(rows + r, 1), :] >= t.astype(F32)
        w0[BW + r, t] = scaled(w0[BW + r, t], BW + r, BW + r + t, keep)
        return c

    def own_lower(i, c):
        r, k = i // BW, i % BW
        keep = reach[pl.ds(r, 1), :] >= (BW - k).astype(F32)
        l0[r, k] = scaled(l0[r, k], BW + r, r + k, keep)
        return c

    def own_diag(r, c):
        w0[BW + r, 0] = scaled_diag(w0[BW + r, 0], BW + r, msg[pl.ds(r, 1), :])
        rd[pl.ds(BW + r, 1), :] = 1.0 / diagonal(w0[BW + r, 0])
        return c

    lax.fori_loop(0, rows, own_diag, 0)
    lax.fori_loop(0, rows * BW, own_upper, 0)
    lax.fori_loop(0, rows * BW, own_lower, 0)

    def above_upper(a):
        def step(t, c):
            keep = above[pl.ds(rows + a, 1), :] >= t.astype(F32)
            w0[a, t] = scaled(w0[a, t], a, a + t, keep)
            return c

        return step

    strict_up, strict_low = col_id > row_id, row_id > col_id

    def keep_if(mask, block):
        return jnp.where(mask, block.astype(F32), 0.0).astype(BF16)

    again = 2 * rows

    def upper_row(r, w, l, w_new, new_row, at):
        own = w[BW + r, 0]
        low = keep_if(strict_low, own)
        pivot = rd[pl.ds(at + BW + r, 1), :]
        for t in range(BW + 1):
            lhs, rhs = [low], [keep_if(strict_up, own) if t == 0 else w[BW + r, t]]
            for m in range(1, BW + 1 - t):
                lhs.append(l[r, BW - m])
                rhs.append(w[BW + r - m, t + m])
            value = w0[BW + r, t].astype(F32) - mm(lhs, rhs)
            if t == 0:
                value = jnp.where(strict_low, value * pivot, value)
            else:
                keep = msg[pl.ds(rows + r, 1), :] >= float(t)
                value = jnp.where(jnp.broadcast_to(keep, (size, size)), value, 0.0)
            w_new[new_row, t] = value.astype(BF16)

    def pack(r, w, row):
        last = w[row, 0, high_half, high_half].astype(F32)
        first = jnp.where(col_half >= row_half, w[row, 0, low_half, low_half].astype(F32), last.T)
        packed[r, :, low_half] = first.astype(BF16)
        packed[r, :, high_half] = w[row, 0, low_half, high_half]
        corner[pl.ds(r, 1), :] = jnp.sum(jnp.where(eye_half, last, 0.0), axis=0, keepdims=True)

    def unpack(r):
        first = w1[r, 0, low_half, low_half].astype(F32)
        values = jnp.broadcast_to(corner_in[pl.ds(r, 1), :], (half, half))
        last = jnp.where(col_half > row_half, first.T, jnp.where(eye_half, values, 0.0))
        w1[r, 0, high_half, high_half] = last.astype(BF16)

    def lower_row(r, w, l, l_new, at):
        for k in range(BW):
            m = BW - k
            lhs, rhs = [l[r, k]], [keep_if(strict_up, w[BW + r - m, 0])]
            for back in range(m + 1, BW + 1):
                lhs.append(l[r, BW - back])
                rhs.append(w[BW + r - back, back - m])
            value = (l0[r, k].astype(F32) - mm(lhs, rhs)) * rd[pl.ds(at + BW + r - m, 1), :]
            keep = reach[pl.ds(r, 1), :] >= float(m)
            l_new[r, k] = jnp.where(jnp.broadcast_to(keep, (size, size)), value, 0.0).astype(BF16)

    def arrive(r, pieces, when):
        for c in range(rows):
            if pieces[c]:

                @pl.when(jnp.logical_and(when, r == c))
                def _():
                    for piece in pieces[c]:
                        piece.wait_recv()

    def by_row(js):
        return [[on_copy(j) for j in js if rest[j][0] == r] for r in range(rows)]

    def rest_kind(count):
        by_link = by_row(range(len(rest) - count))
        by_link[0].append(x_rest(from_first, 0, BW - count, BW))
        return by_link

    rest_kinds = (
        (jnp.logical_and(from_relay, grp > 0), rest_kind(DIRECT)),
        (edge_in, rest_kind(DIRECT_EDGE)),
    )
    beside_rest = [[x_rest(from_first, r, 0, BW - r)] for r in range(rows)]
    x_first = [[x_crit(from_first, r, BW + 1)] for r in range(rows)]
    x_first_edge = [[x_crit(from_first, r, BW)] if r else [] for r in range(rows)]
    y_first = [[y_part(w1.at[BW + r], r, 0)] if r else [] for r in range(rows)]
    y_rest = [[y_part(w1.at[BW + r], r, kind) for kind in ((1, 2) if r < rows - 1 else (2,))] for r in range(rows)]
    y_rest[rows - 1].append(corner_copy)
    y_last, y_rest[0] = y_rest[0], []
    y_last_edge = y_edge() + [y_part(w1.at[BW], 0, 2)] + [side_on(k) for k in range(1, n_side + 1)]

    @pl.when(edge_in)
    def _():
        for copy in g_copies:
            copy.wait_recv()

    def last_column(r, diag_block, old):
        keep = above[pl.ds(rows + r, 1), :] >= float(BW)
        value = base[r].astype(F32) - mm([keep_if(strict_low, diag_block)], [old])
        return jnp.where(jnp.broadcast_to(keep, (size, size)), value, 0.0).astype(BF16)

    def upper_1(i, c):
        r = rows - 1 - i
        arrive(r, x_first, grp > 0)
        arrive(r, x_first_edge, edge_in)

        @pl.when(grp > 0)
        def _():
            lax.fori_loop(BW - r, BW + 1, above_upper(r), 0)
            base[r] = w0[r, BW]

        @pl.when(grp == 0)
        def _():
            keep = above[pl.ds(rows + r, 1), :] >= float(BW)
            base[r] = scaled(base[r], r, r + BW, keep)
            first = diag0[r, :, low_half].astype(F32)
            top = jnp.concatenate([first, jnp.zeros((half, half), F32)], axis=1)
            bottom = jnp.concatenate([diag0[r, :, high_half].astype(F32), first.T], axis=1)
            first_diag = scaled_diag(jnp.concatenate([top, bottom], axis=0), r, above[pl.ds(r, 1), :])
            w0[r, BW] = last_column(r, first_diag, base[r])

        upper_row(r, w0, l0, w1, BW + r, 0)
        rd[pl.ds(again + BW + r, 1), :] = 1.0 / diagonal(w1[BW + r, 0])
        pack(r, w1, BW + r)
        return c

    @pl.when(jnp.logical_not(has_prev))
    def _():
        def clear(a, c):
            base[a] = jnp.zeros((size, size), BF16)
            diag0[a] = jnp.zeros((half, size), BF16)
            return c

        lax.fori_loop(0, rows, clear, 0)

    lax.fori_loop(0, rows, upper_1, 0)

    @pl.when(jnp.logical_not(odd))
    def _():
        for part in y_parts(lambda r: w1.at[BW + r]):
            part.start()

    @pl.when(edge_out)
    def _():
        for r in range(rows - 1, 0, -1):
            x_crit(from_first, r, BW).start()
        for j in range(n_edge):
            out_copy(j).start()
        x_rest(from_first, 0, BW - DIRECT_EDGE, BW).start()

    def lower_1(i, c):
        r = rows - 1 - i
        arrive(r, beside_rest, odd)
        for kind, pieces in rest_kinds:
            arrive(r, pieces, kind)

        @pl.when(grp > 0)
        def _():
            w0[r, 0] = scaled_diag(w0[r, 0], r, above[pl.ds(r, 1), :])
            lax.fori_loop(1, BW - r, above_upper(r), 0)

        rd[pl.ds(r, 1), :] = 1.0 / diagonal(w0[r, 0])
        lower_row(r, w0, l0, l1, 0)
        return c

    @pl.when(odd)
    def _():
        lax.fori_loop(0, rows, lower_1, 0)

    n_most = max(n_plain, n_edge)
    half_way = n_most // 2
    forward(range(half_way))

    @pl.when(inside_odd)
    def _():
        x_rest(from_input, 0, BW - DIRECT, BW).start()
        for part in y_parts(lambda r: w1.at[BW + r]):
            part.start()

    forward(range(half_way, n_most))

    def upper_2(i, c):
        r = rows - 1 - i
        arrive(r, y_first, has_prev)
        w1[r, BW] = last_column(r, w0[r, 0], w0[r, BW])
        upper_row(r, w1, l1, wo, r, again)

        @pl.when(edge_out)
        def _():
            pack(r, wo, r)

        return c

    def lower_2(i, c):
        r = rows - 1 - i
        arrive(r, y_rest, has_prev)
        arrive(r, [y_last] + [[]] * (rows - 1), grp > 0)
        arrive(r, [y_last_edge] + [[]] * (rows - 1), edge_in)

        @pl.when(has_prev)
        def _():
            unpack(r)

        rd[pl.ds(again + r, 1), :] = 1.0 / diagonal(w1[r, 0])
        lower_row(r, w1, l1, lo, again)
        return c

    for k in range(1, n_side + 1):

        @pl.when(jnp.logical_and(on_side, side_back == k))
        def _():
            side_out(k).wait_recv()
            side_on(k).start()

    @pl.when(odd)
    def _():
        lax.fori_loop(0, rows, upper_2, 0)

    @pl.when(edge_out)
    def _():
        for k in range(1, n_side + 1):
            side_out(k).start()
        for part in y_parts_edge():
            part.start()

    def finish(i, c):
        @pl.when(jnp.logical_not(odd))
        def _():
            lower_1(i, c)
            upper_2(i, c)

        lower_2(i, c)
        return c

    lax.fori_loop(0, rows, finish, 0)

    @pl.when(has_next)
    def _():
        to_next.wait_send()

    for k in range(1, n_side + 1):

        @pl.when(jnp.logical_and(on_side, side_back == k))
        def _():
            side_on(k).wait_send()

    @pl.when(inside)
    def _():
        for part in y_parts(lambda r: w1.at[BW + r]):
            part.wait_send()
        for r in downward:
            x_crit(from_first, r, BW + 1).wait_send()

    @pl.when(jnp.logical_not(odd))
    def _():
        for r in downward:
            x_rest(from_first, r, 0, BW - r).wait_send()

    @pl.when(inside_odd)
    def _():
        for j in range(n_plain):
            out_copy(j).wait_send()
        x_rest(from_first, 0, BW - DIRECT, BW).wait_send()

    @pl.when(edge_out)
    def _():
        for k in range(1, n_side + 1):
            side_out(k).wait_send()
        for part in y_parts_edge():
            part.wait_send()
        for copy in g_copies:
            copy.wait_send()
        for r in range(rows - 1, 0, -1):
            x_crit(from_first, r, BW).wait_send()
        for j in range(n_edge):
            out_copy(j).wait_send()
        x_rest(from_first, 0, BW - DIRECT_EDGE, BW).wait_send()

    for kind, count in by_kind:

        @pl.when(kind)
        def _():
            for j in range(count):
                on_copy(j).wait_send()

    @pl.when(has_prev)
    def _():
        to_prev.wait_send()


def per_device(n_slab, n_grp, blocks, diag_shift, offsets):
    rows, band, size, _ = blocks.shape
    block = (size, size)
    n_rest = BW * (BW + 1) // 2
    call = pl.pallas_call(
        functools.partial(kernel, n_slab, n_grp),
        out_shape=pltpu.VMEM(blocks.shape, BF16),
        in_specs=[
            pl.BlockSpec(memory_space=pltpu.HBM),
            pl.BlockSpec(memory_space=pltpu.HBM),
            pl.BlockSpec(memory_space=pltpu.HBM),
        ],
        out_specs=pl.BlockSpec(memory_space=pltpu.VMEM),
        scratch_shapes=[
            pltpu.VMEM((2 * rows, BW + 1) + block, BF16),
            pltpu.VMEM((rows, BW) + block, BF16),
            pltpu.VMEM((2 * rows, BW + 1) + block, BF16),
            pltpu.VMEM((rows, BW) + block, BF16),
            pltpu.VMEM((rows,) + block, BF16),
            pltpu.VMEM((rows, size // 2, size), BF16),
            pltpu.VMEM((rows, size // 2, size), BF16),
            pltpu.VMEM((1,) + block, BF16),
            pltpu.VMEM((n_rest,) + block, BF16),
            pltpu.VMEM((rows, size // 2, size), BF16),
            pltpu.VMEM((2 * rows, size // 2), F32),
            pltpu.VMEM((2 * rows, size // 2), F32),
            pltpu.VMEM((rows * size,), F32),
            pltpu.VMEM((2, rows), jnp.int32),
            pltpu.VMEM((2 * rows, size), F32),
            pltpu.VMEM((2 * rows, size), F32),
            pltpu.VMEM((2 * rows, size), F32),
            pltpu.VMEM((2 * rows, size), F32),
            pltpu.VMEM((4 * rows, size), F32),
            pltpu.VMEM((2 * rows, size, LANES), F32),
            pltpu.VMEM((4 * rows, size), F32),
            pltpu.SemaphoreType.DMA((5,)),
            pltpu.SemaphoreType.DMA((2,)),
            pltpu.SemaphoreType.DMA((2,)),
            pltpu.SemaphoreType.DMA((2 * rows,)),
            pltpu.SemaphoreType.DMA((2 * rows,)),
            pltpu.SemaphoreType.DMA((4 * rows,)),
            pltpu.SemaphoreType.DMA((4 * rows,)),
            pltpu.SemaphoreType.DMA((3,)),
            pltpu.SemaphoreType.DMA((3,)),
        ] + [pltpu.SemaphoreType.DMA((n_rest,))] * 4 + [pltpu.SemaphoreType.DMA((rows,))] * 4,
        compiler_params=pltpu.CompilerParams(
            collective_id=0, has_side_effects=True, vmem_limit_bytes=67_043_328 - 2 * blocks.size
        ),
        name="sweeps",
    )
    return call(blocks, diag_shift, offsets.T)


def solution(mesh):
    return jax.shard_map(
        functools.partial(per_device, mesh.shape["slab"], mesh.shape["grp"]),
        mesh=mesh,
        in_specs=(
            P(("slab", "grp"), None, None, None),
            P(("slab", "grp")),
            P(("slab", "grp"), None),
        ),
        out_specs=P(("slab", "grp"), None, None, None),
        check_vma=False,
    )
```
